32 devices in a mesh: row: 8 (over z, y), col: 4 (over x, core).
Axes of the slice: x: 2, y: 2, z: 4, core: 2. Of those that a mesh axis runs over, the one named last changes fastest.
Arguments:
- embeddings: bfloat16 [12288, 768], P(('row', 'col'))
- doc_order: int32 [12288], P(('row', 'col')), may hold values from 0 to 12287, each once
Outputs:
- nearest_earlier: float32 [12288], P(('row', 'col'))
The draws below stay inside these ranges and needn't reach their ends.
Inputs may be any that keep to these rules, and one draw needn't show every extreme that they name: `doc_order`: each value 0 to 12287 appears once.
All inputs are finite; a program needn't handle non-finite values.
Results may differ from the reference program's by a relative error of at most 0.00051.
Values may be sent and summed in bfloat16 or wider, within the bound.
A program may use at most 64 MiB of HBM per device.

```python
import jax
import jax.numpy as jnp
from jax import lax

D = 768
N = 12288


def draw_embeddings(key, part):
    groups = max(N // 4, 1)
    key_group = jax.random.fold_in(key, 11)
    key_amp = jax.random.fold_in(key, 12)
    key_center = jax.random.fold_in(key, 13)
    key_noise = jax.random.fold_in(key, 14)
    member = jax.random.randint(key_group, (N,), 0, groups)
    amplitude = jax.random.uniform(key_amp, (groups,), jnp.float32, 0.5, 3.0)
    centers = jax.random.normal(key_center, (groups, D), jnp.float32)
    noise = jax.random.normal(key_noise, (N, D), jnp.float32)
    values = noise + amplitude[member][:, None] * centers[member]
    return values.astype(jnp.bfloat16)


def setup_inputs(seed: int = 0) -> dict:
    streams_of = jax.random.split(jax.random.key(seed), 3)
    embeddings = draw_embeddings(jax.random.fold_in(streams_of[2], 71), 0)
    doc_order = jax.random.permutation(streams_of[1], N).astype(jnp.int32)
    return dict(embeddings=embeddings, doc_order=doc_order)


def normalize_rows(embeddings):
    floats = embeddings.astype(jnp.float32)
    scale = lax.rsqrt(lax.optimization_barrier(jnp.sum(floats * floats, axis=1, keepdims=True)) + 1e-06)
    return (floats * scale).astype(jnp.bfloat16)

def reference(embeddings, doc_order):
    unit_rows = normalize_rows(embeddings)
    block_rows = 1024 if N % 1024 == 0 else N
    row_groups = unit_rows.reshape(N // block_rows, block_rows, D)
    order_groups = doc_order.reshape(N // block_rows, block_rows)

    def one_block(pair):
        rows_here, orders_here = pair
        scores = jnp.dot(rows_here, unit_rows.T, preferred_element_type=jnp.float32)
        earlier = doc_order[None, :] < orders_here[:, None]
        masked = jnp.where(earlier, scores, jnp.float32(-1.0))
        return jnp.maximum(lax.optimization_barrier(jnp.max(masked, axis=1)), jnp.float32(-1.0))
    result = lax.map(one_block, (row_groups, order_groups))
    return result.reshape(N)
```

```python
import functools

import jax
import jax.numpy as jnp
from jax import lax
from jax.experimental import pallas as pl
from jax.experimental.pallas import tpu as pltpu
from jax.sharding import PartitionSpec as P

MESH = pl.DeviceIdType.MESH
LANES = 128
PIECE = 64


def fast_size(rows):
    best = 1
    for size in range(1, rows + 1):
        if rows % size == 0 and size * size <= rows:
            best = size
    return best


class Layout:
    def __init__(self, rows, cols):
        self.fast = fast_size(rows)
        self.slow = rows // self.fast
        self.cores = 2 if cols % 2 == 0 else 1
        self.xs = cols // self.cores
        self.chips = self.fast * self.xs
        self.plane = self.chips * self.cores
        self.down = self.slow > 2
        self.slots = max(self.slow - 2, 1) + 1
        chips = [(f, x) for f in range(self.fast) for x in range(self.xs)]
        near = [c for c in chips if (c[0] == 0) != (c[1] == 0)]
        far = [c for c in chips if c[0] != 0 and c[1] != 0]
        self.offsets = near + far
        self.near = list(range(len(near)))
        self.far = list(range(len(near), len(near) + len(far)))


def kernel(
    lay, n, chunks,
    emb, order, out,
    raw, own_order, units, line, orders, line_orders, col_orders,
    row_best, col_best, plane_res, line_res, plane_in, line_in,
    load, ps, pr, fr, sr, ls, lr, os_, or_, osr, los, lor, rs, rr, lrs, lrr,
):
    S, F, X, C = lay.slow, lay.fast, lay.xs, lay.cores
    own = lay.slots
    last = S - 1
    rows_here = n // chunks
    align = PIECE if rows_here % PIECE == 0 else rows_here
    r, c = lax.axis_index("row"), lax.axis_index("col")
    z, f = r // F, lax.rem(r, F)
    x, core = c // C, lax.rem(c, C)
    chip = f * X + x
    slot = chip * C + core

    def plane_id(df, dx, dc):
        return {
            "row": z * F + lax.rem(f + df, F),
            "col": lax.rem(x + dx, X) * C + lax.rem(core + dc, C),
        }

    def line_id(there):
        return {"row": there * F + f, "col": c}

    def source_chip(df, dx):
        return lax.rem(f + F - df, F) * X + lax.rem(x + X - dx, X)

    def span(which, k, count=1):
        return pl.ds(pl.multiple_of(which * n + k * rows_here, align), count * rows_here)

    def remote(src, dst, send, recv, where):
        return pltpu.make_async_remote_copy(
            src_ref=src, dst_ref=dst, send_sem=send, recv_sem=recv,
            device_id=where, device_id_type=MESH,
        )

    def here(part, sem):
        return remote(part, part, sem, sem, plane_id(0, 0, 1))

    pairs = [(k, min(2, chunks - k)) for k in range(0, chunks, 2)]

    def plane_copy(i, k):
        part = units.at[span(slot, k)]
        return remote(part, part, ps, pr.at[i, k], plane_id(*lay.offsets[i], 0))

    def relay_copy(i, k):
        df, dx = lay.offsets[i]
        src, step = ((0, dx), (df, 0)) if k % 2 == 0 else ((df, 0), (0, dx))
        part = units.at[span(source_chip(*src) * C + core, k)]
        return remote(part, part, ps, fr.at[i - len(lay.near), k // 2], plane_id(*step, 0))

    def sibling_copy(i, k, count):
        src = chip if i < 0 else source_chip(*lay.offsets[i])
        part = units.at[span(src * C + core, k, count)]
        return remote(part, part, ps, sr.at[i + 1], plane_id(0, 0, 1))

    def near_wait(i, k):
        src = source_chip(*lay.offsets[i]) * C + core
        here(units.at[span(src, k)], pr.at[i, k]).wait_recv()

    def far_wait(i, g):
        src = source_chip(*lay.offsets[i]) * C + core
        k, count = pairs[g]
        here(units.at[span(src, k, count)], fr.at[i - len(lay.near), g]).wait_recv()

    def sibling_wait(i):
        src = chip if i < 0 else source_chip(*lay.offsets[i])
        part = units.at[span(src * C + lax.rem(core + 1, C), 0, chunks)]
        here(part, sr.at[i + 1]).wait_recv()

    sends_up = z < last
    relays_up = (z > 0) & (z < S - 2)
    sends_down = z == last
    transit = z < last
    relays_down = (z > 0) & (z < last)

    def meets(src, dst):
        found = ((src < dst) & (dst < last)) | ((src == last - 1) & (dst == last))
        if lay.down:
            found = found | ((src == last) & (dst < last - 1))
        return found

    def source(w):
        return last if w == 0 else z - w

    def valid(w):
        if w == 0:
            return z < last - 1
        found = (z >= w) & (z < last)
        return (found | (z == last)) if w == 1 else found

    def line_copy(src, k, dst_slot, tag, there):
        return remote(
            src, line.at[dst_slot, pl.ds(k * rows_here, rows_here)],
            ls.at[tag], lr.at[dst_slot, k], line_id(there),
        )

    def own_part(k):
        return units.at[span(slot, k)]

    def slot_part(w, k):
        return line.at[w, pl.ds(k * rows_here, rows_here)]

    def own_up(k):
        return line_copy(own_part(k), k, 1, 0, z + 1)

    def own_down(k):
        return line_copy(own_part(k), k, 0, 0, z - 1)

    def relay_up(w, k):
        return line_copy(slot_part(w, k), k, w + 1, 1 + w, z + 1)

    def relay_down(k):
        return line_copy(slot_part(0, k), k, 0, 1, z - 1)

    def line_wait(w, k):
        here(slot_part(w, k), lr.at[w, k]).wait_recv()

    def line_order(src, dst_slot, tag, there):
        return remote(src, line_orders.at[dst_slot], los.at[tag], lor.at[dst_slot], line_id(there))

    def order_up():
        return line_order(orders.at[slot], 1, 0, z + 1)

    def order_down():
        return line_order(orders.at[slot], 0, 0, z - 1)

    def order_on_up(w):
        return line_order(line_orders.at[w], w + 1, 1 + w, z + 1)

    def order_on_down():
        return line_order(line_orders.at[0], 0, 1, z - 1)

    def order_send(src, sem, where):
        return remote(orders.at[src], orders.at[src], os_, sem, where)

    def order_copy(i):
        return order_send(slot, or_.at[i], plane_id(*lay.offsets[i], 0))

    def order_relay(i):
        df, dx = lay.offsets[i]
        return order_send(source_chip(0, dx) * C + core, or_.at[i], plane_id(df, 0, 0))

    def order_wait(i):
        src = source_chip(*lay.offsets[i]) * C + core
        here(orders.at[src], or_.at[i]).wait_recv()

    def order_across(i):
        src = chip if i < 0 else source_chip(*lay.offsets[i])
        return order_send(src * C + core, osr.at[i + 1], plane_id(0, 0, 1))

    def order_across_wait(i):
        src = chip if i < 0 else source_chip(*lay.offsets[i])
        here(orders.at[src * C + lax.rem(core + 1, C)], osr.at[i + 1]).wait_recv()

    barrier = pltpu.get_barrier_semaphore()
    steps = [(*lay.offsets[i], 0) for i in lay.near] + ([(0, 0, 1)] if C > 1 else [])
    sides = ((z > 0, z - 1), (z < last, z + 1))
    for step in steps:
        pl.semaphore_signal(barrier, inc=1, device_id=plane_id(*step), device_id_type=MESH)
    for there, which in sides:
        pl.when(there)(
            lambda which=which: pl.semaphore_signal(
                barrier, inc=1, device_id=line_id(which), device_id_type=MESH
            )
        )
    loads = [
        pltpu.make_async_copy(emb, raw, load.at[0]),
        pltpu.make_async_copy(order, own_order, load.at[1]),
    ]
    for one in loads:
        one.start()
    row_best[...] = jnp.full(row_best.shape, -1.0, jnp.float32)
    col_best[...] = jnp.full(col_best.shape, -1.0, jnp.float32)
    loads[1].wait()
    orders[pl.ds(slot, 1)] = own_order[...].reshape(1, 1, n)
    loads[0].wait()

    def normalize(k):
        floats = raw[pl.ds(k * rows_here, rows_here), :].astype(jnp.float32)
        scale = lax.rsqrt(jnp.sum(floats * floats, axis=1, keepdims=True) + 1e-06)
        units[span(slot, k), :] = (floats * scale).astype(jnp.bfloat16)

    for k in range(chunks):
        normalize(k)
    lines = jnp.minimum(z, 1) + jnp.minimum(last - z, 1)
    pl.semaphore_wait(barrier, len(steps) + lines)

    def start(cond, *copies):
        @pl.when(cond)
        def run():
            for one in copies:
                one().start()

    early = (chunks + 1) // 2
    if S > 1:
        start(sends_up, order_up, *[functools.partial(own_up, k) for k in range(early)])
        start(sends_up & jnp.logical_not(relays_up),
              *[functools.partial(own_up, k) for k in range(early, chunks)])
    if lay.down:
        start(sends_down, order_down, *[functools.partial(own_down, k) for k in range(chunks)])
    for i in lay.near:
        order_copy(i).start()
    if C > 1:
        order_across(-1).start()
        sibling_copy(-1, 0, chunks).start()
    for k in range(chunks):
        for i in lay.near:
            plane_copy(i, k).start()

    def spread(which, row):
        wide = jnp.broadcast_to(row.reshape(1, n), (LANES, n))
        col_orders[which] = wide.T

    spread(own, orders[slot])

    width = C * n

    def item(lhs, w, first_chip, both, first=0, count=n, wide=1):
        rhs = units[pl.ds(pl.multiple_of(first_chip * width, LANES), wide * width), :]
        s = lax.dot_general(
            lhs, rhs, (((1,), (1,)), ((), ())), preferred_element_type=jnp.float32
        )
        mine = col_orders[w, first:first + count, :]
        rows_max = None
        for j in range(wide * width // LANES):
            part = s[:, j * LANES:(j + 1) * LANES]
            which_chip, at = first_chip + j * LANES // width, j * LANES % width
            core_at, lane_at = at // n, at % n
            theirs = orders[which_chip * C + core_at, :, lane_at:lane_at + LANES]
            earlier = theirs < mine
            if both:
                cand = jnp.where(earlier, part, jnp.float32(-1.0))
                rows_max = cand if rows_max is None else jnp.maximum(rows_max, cand)
                later = jnp.where(earlier, jnp.float32(-1.0), part)
            else:
                later = jnp.where(mine < theirs, part, jnp.float32(-1.0))
            down = jnp.max(later.reshape(count // 8, 8, LANES), axis=0)
            col_best[which_chip, :, at:at + LANES] = jnp.maximum(
                col_best[which_chip, :, at:at + LANES], down
            )
        if both:
            row_best[w, first:first + count, :] = jnp.maximum(
                row_best[w, first:first + count, :], rows_max
            )

    def own_item(which_chip):
        lhs = units[pl.ds(pl.multiple_of(slot * n, LANES), n), :]
        item(lhs, own, which_chip, False)

    def chips_of(places):
        def at(j):
            if places == "near":
                by_x = j < X - 1
                df = jnp.where(by_x, 0, j - (X - 2))
                dx = jnp.where(by_x, j + 1, 0)
            elif places == "far":
                df, dx = 1 + j // max(X - 1, 1), 1 + lax.rem(j, max(X - 1, 1))
            else:
                df, dx = 0, 0
            return source_chip(df, dx)

        return {"near": F + X - 2, "far": (F - 1) * (X - 1), "self": 1}[places], at

    def loop(places, body):
        count, at = chips_of(places)

        def step(j, carry):
            body(at(j))
            return carry

        if count == 1:
            body(at(0))
        elif count:
            lax.fori_loop(0, count, step, 0)

    def line_sweep(w, places, first, count, cond):
        @pl.when(valid(w) & cond)
        def run():
            loop(places, lambda one: item(
                line[w, first:first + count, :], w, one, True, first, count
            ))

    wide = next(m for m in (4, 3, 2, 1) if lay.chips % m == 0)

    def wide_sweep(w, first, count, cond):
        def body(j, carry):
            item(line[w, first:first + count, :], w, j * wide, True, first, count, wide)
            return carry

        @pl.when(valid(w) & cond)
        def run():
            lax.fori_loop(0, lay.chips // wide, body, 0)

    for i in lay.near:
        order_wait(i)
        if C > 1:
            order_across(i).start()
    for i in lay.far:
        order_relay(i).start()

    def take_order(w):
        if w == 0 and not lay.down:
            return
        arrives = transit if w == 0 else valid(w)

        @pl.when(arrives)
        def run():
            here(line_orders.at[w], lor.at[w]).wait_recv()
            if w == 0:
                pl.when(relays_down)(lambda: order_on_down().start())
            elif w < S - 2:
                pl.when(relays_up)(lambda: order_on_up(w).start())

        pl.when(valid(w))(lambda: spread(w, line_orders[w]))

    if S > 1:
        take_order(1)
    if C > 1:
        order_across_wait(-1)
        sibling_wait(-1)
    own_item(chip)
    if C > 1:
        for i in lay.near:
            order_across_wait(i)

    held = (z > 1) & (z < last) if S > 3 else z < 0
    straight = jnp.logical_not(held)
    half = early * rows_here

    def take_first(k):
        cond = valid(1) if k < early else valid(1) & straight

        @pl.when(cond)
        def run():
            line_wait(1, k)
            if S > 3:
                pl.when(relays_up)(lambda: relay_up(1, k).start())

    def take_last(k):
        @pl.when(valid(1) & held)
        def run():
            line_wait(1, k)
            if S > 4:
                pl.when(relays_up)(lambda: relay_up(1, k).start())

    def take_down(p):
        if not lay.down:
            return
        for there in range(S - 2, 0, -1):
            k = p - 2 * (S - 2 - there)
            if 0 <= k < chunks:
                @pl.when(z == there)
                def run(k=k):
                    line_wait(0, k)
                    relay_down(k).start()

    for k in range(chunks):
        if S > 1:
            take_first(k)
        for i in lay.near:
            near_wait(i, k)
        for i in lay.far:
            relay_copy(i, k).start()
        if C > 1:
            for i in lay.near:
                sibling_copy(i, k, 1).start()
        if k == 0:
            take_order(0)
        take_down(k)
    if S > 3:
        start(relays_up, *[functools.partial(own_up, k) for k in range(early, chunks)])

    def far_group(g):
        for i in lay.far:
            far_wait(i, g)
            if C > 1:
                sibling_copy(i, *pairs[g]).start()

    always = z >= 0
    if C > 1:
        for i in lay.near:
            sibling_wait(i)
    loop("near", own_item)
    more = list(range(chunks, chunks + 2 * max(S - 3, 0)))
    for p in more[:1]:
        take_down(p)
    for i in lay.far:
        order_wait(i)
        if C > 1:
            order_across(i).start()
    far_group(0)
    if S > 1:
        line_sweep(1, "self", 0, n, straight)
        if S > 3:
            line_sweep(1, "self", 0, half, held)
    for p in more[1:]:
        take_down(p)
    if S > 1:
        line_sweep(1, "near", 0, n, straight)
        if S > 3:
            line_sweep(1, "near", 0, half, held)
    for g in range(1, len(pairs)):
        far_group(g)

    if lay.down:
        @pl.when(z == 0)
        def run():
            for k in range(chunks):
                line_wait(0, k)
        line_sweep(0, "self", 0, n, always)
        line_sweep(0, "near", 0, n, always)
    for w in range(2, S - 1):
        @pl.when(valid(w))
        def run(w=w):
            for k in range(chunks):
                line_wait(w, k)
                if w < S - 2:
                    pl.when(z < S - 2)(lambda: relay_up(w, k).start())
            here(line_orders.at[w], lor.at[w]).wait_recv()
            if w < S - 2:
                pl.when(z < S - 2)(lambda: order_on_up(w).start())
            spread(w, line_orders[w])
        line_sweep(w, "self", 0, n, always)
        line_sweep(w, "near", 0, n, always)

    if C > 1:
        for i in lay.far:
            order_across_wait(i)
            sibling_wait(i)
    loop("far", own_item)
    order_of_slots = ([0] if lay.down else []) + list(range(2, S - 1))
    for w in order_of_slots:
        line_sweep(w, "far", 0, n, always)
    if S > 1:
        line_sweep(1, "far", 0, n, straight)
        if S > 3:
            line_sweep(1, "far", 0, half, held)

    def line_result(w):
        return remote(line_res.at[w], line_in.at[z], lrs.at[w], lrr.at[z], line_id(source(w)))

    def give_back(w, cond):
        @pl.when(valid(w) & cond)
        def fold():
            line_res[w] = jnp.max(row_best[w].T, axis=0, keepdims=True)
            line_result(w).start()

    for w in order_of_slots:
        give_back(w, always)
    if S > 1:
        give_back(1, straight)
    if S > 3:
        for k in range(early, chunks - 1):
            take_last(k)
        if chunks - 1 > early:
            wide_sweep(1, half, (chunks - 1 - early) * rows_here, held)
        if chunks > early:
            take_last(chunks - 1)
            wide_sweep(1, (chunks - 1) * rows_here, rows_here, held)
        give_back(1, held)

    def result_copy(df, dx, dc):
        there = (lax.rem(f + df, F) * X + lax.rem(x + dx, X)) * C + lax.rem(core + dc, C)
        o = (df * X + dx) * C + dc
        return remote(plane_res.at[there], plane_in.at[o], rs, rr, plane_id(df, dx, dc))

    def flush(df, dx):
        one = lax.rem(f + df, F) * X + lax.rem(x + dx, X)
        flat = jnp.max(col_best[one], axis=0, keepdims=True)
        for core_at in range(C):
            plane_res[one * C + core_at] = flat[:, core_at * n:(core_at + 1) * n]

    def flush_out(j, carry):
        df, dx = (lay.chips - 1 - j) // X, lax.rem(lay.chips - 1 - j, X)
        flush(df, dx)
        for dc in range(C):
            result_copy(df, dx, dc).start()
        return carry

    lax.fori_loop(0, lay.chips - 1, flush_out, 0)
    flush(0, 0)
    if C > 1:
        result_copy(0, 0, 1).start()

    best = jnp.maximum(plane_res[slot], jnp.float32(-1.0))
    if lay.plane > 1:
        here(plane_in.at[pl.ds(1, lay.plane - 1)], rr).wait_recv()
        best = jnp.maximum(best, jnp.max(plane_in[1:], axis=0))
    plane_res[slot] = best
    for src in range(S):
        def gather(src=src):
            here(line_in.at[src], lrr.at[src]).wait_recv()
            plane_res[slot] = jnp.maximum(plane_res[slot], line_in[src])

        pl.when(meets(z, jnp.int32(src)))(gather)
    out[...] = plane_res[slot].reshape(n)

    def sent(part, sem):
        here(part, sem).wait_send()

    if lay.plane > 1:
        sent(units.at[pl.ds(0, (lay.plane - 1) * n)], ps)
        sent(orders.at[pl.ds(0, lay.plane - 1)], os_)
        sent(plane_in.at[pl.ds(1, lay.plane - 1)], rs)

    def line_sent(cond, tag):
        @pl.when(cond)
        def run():
            sent(line.at[0], ls.at[tag])
            sent(line_orders.at[0], los.at[tag])

    if S > 1:
        line_sent((sends_up | sends_down) if lay.down else sends_up, 0)
    if lay.down:
        line_sent(relays_down, 1)
    for w in range(1, S - 2):
        line_sent(valid(w) & (z < S - 2), 1 + w)
    for w in range(lay.slots):
        if S > 1 and (w or lay.down):
            pl.when(valid(w))(lambda w=w: sent(line_res.at[w], lrs.at[w]))


def shards(lay, embeddings, doc_order):
    n, depth = embeddings.shape
    chunks = n // PIECE if n % PIECE == 0 else 1
    dma = pltpu.SemaphoreType.DMA
    S, near, far = lay.slow, max(len(lay.near), 1), max(len(lay.far), 1)
    vmem = pltpu.VMEM
    return pl.pallas_call(
        functools.partial(kernel, lay, n, chunks),
        out_shape=vmem((n,), jnp.float32),
        in_specs=[pl.BlockSpec(memory_space=pl.ANY)] * 2,
        out_specs=pl.BlockSpec(memory_space=vmem),
        scratch_shapes=[
            vmem((n, depth), jnp.bfloat16),
            vmem((n,), jnp.int32),
            vmem((lay.plane * n, depth), jnp.bfloat16),
            vmem((lay.slots, n, depth), jnp.bfloat16),
            vmem((lay.plane, 1, n), jnp.int32),
            vmem((lay.slots, 1, n), jnp.int32),
            vmem((lay.slots + 1, n, LANES), jnp.int32),
            vmem((lay.slots, n, LANES), jnp.float32),
            vmem((lay.chips, 8, lay.cores * n), jnp.float32),
            vmem((lay.plane, 1, n), jnp.float32),
            vmem((lay.slots, 1, n), jnp.float32),
            vmem((lay.plane, 1, n), jnp.float32),
            vmem((S, 1, n), jnp.float32),
            dma((2,)),
            dma(()), dma((near, chunks)), dma((far, (chunks + 1) // 2)), dma((near + far + 1,)),
            dma((S,)), dma((lay.slots, chunks)),
            dma(()), dma((near + far,)), dma((near + far + 1,)),
            dma((S,)), dma((lay.slots,)),
            dma(()), dma(()),
            dma((lay.slots,)), dma((S,)),
        ],
        compiler_params=pltpu.CompilerParams(
            collective_id=0, has_side_effects=True, vmem_limit_bytes=60 * 1024 * 1024
        ),
    )(embeddings, doc_order)


def solution(mesh):
    lay = Layout(mesh.shape["row"], mesh.shape["col"])
    return jax.shard_map(
        functools.partial(shards, lay),
        mesh=mesh,
        in_specs=(P(("row", "col"), None), P(("row", "col"))),
        out_specs=P(("row", "col")),
        check_vma=False,
    )
```

```python
import functools

import jax
import jax.numpy as jnp
from jax import lax
from jax.experimental import pallas as pl
from jax.experimental.pallas import tpu as pltpu
from jax.sharding import PartitionSpec as P

MESH = pl.DeviceIdType.MESH
LANES = 128
PIECE = 64


def fast_size(rows):
    best = 1
    for size in range(1, rows + 1):
        if rows % size == 0 and size * size <= rows:
            best = size
    return best


class Layout:
    def __init__(self, rows, cols):
        self.fast = fast_size(rows)
        self.slow = rows // self.fast
        self.cores = 2 if cols % 2 == 0 else 1
        self.xs = cols // self.cores
        self.chips = self.fast * self.xs
        self.plane = self.chips * self.cores
        self.down = self.slow > 2
        self.slots = max(self.slow - 2, 1) + 1
        self.hold = self.slow == 4
        chips = [(f, x) for f in range(self.fast) for x in range(self.xs)]
        near = [c for c in chips if (c[0] == 0) != (c[1] == 0)]
        far = [c for c in chips if c[0] != 0 and c[1] != 0]
        self.offsets = near + far
        self.near = list(range(len(near)))
        self.far = list(range(len(near), len(near) + len(far)))


def kernel(
    lay, n, chunks,
    emb, order, out,
    raw, own_order, units, line, orders, line_orders, col_orders,
    row_best, col_best, plane_res, line_res, plane_in, line_in,
    load, ps, pr, fr, sr, ls, lr, os_, or_, osr, los, lor, rs, rr, lrs, lrr,
):
    S, F, X, C = lay.slow, lay.fast, lay.xs, lay.cores
    own = lay.slots
    last = S - 1
    rows_here = n // chunks
    align = PIECE if rows_here % PIECE == 0 else rows_here
    r, c = lax.axis_index("row"), lax.axis_index("col")
    z, f = r // F, lax.rem(r, F)
    x, core = c // C, lax.rem(c, C)
    chip = f * X + x
    slot = chip * C + core

    def plane_id(df, dx, dc):
        return {
            "row": z * F + lax.rem(f + df, F),
            "col": lax.rem(x + dx, X) * C + lax.rem(core + dc, C),
        }

    def line_id(there):
        return {"row": there * F + f, "col": c}

    def source_chip(df, dx):
        return lax.rem(f + F - df, F) * X + lax.rem(x + X - dx, X)

    def span(which, k, count=1):
        return pl.ds(pl.multiple_of(which * n + k * rows_here, align), count * rows_here)

    def remote(src, dst, send, recv, where):
        return pltpu.make_async_remote_copy(
            src_ref=src, dst_ref=dst, send_sem=send, recv_sem=recv,
            device_id=where, device_id_type=MESH,
        )

    def here(part, sem):
        return remote(part, part, sem, sem, plane_id(0, 0, 1))

    pairs = [(k, min(2, chunks - k)) for k in range(0, chunks, 2)]

    def plane_copy(i, k):
        part = units.at[span(slot, k)]
        return remote(part, part, ps, pr.at[i, k], plane_id(*lay.offsets[i], 0))

    def relay_copy(i, k):
        df, dx = lay.offsets[i]
        src, step = ((0, dx), (df, 0)) if k % 2 == 0 else ((df, 0), (0, dx))
        part = units.at[span(source_chip(*src) * C + core, k)]
        return remote(part, part, ps, fr.at[i - len(lay.near), k // 2], plane_id(*step, 0))

    def sibling_copy(i, k, count):
        src = chip if i < 0 else source_chip(*lay.offsets[i])
        part = units.at[span(src * C + core, k, count)]
        return remote(part, part, ps, sr.at[i + 1], plane_id(0, 0, 1))

    def near_wait(i, k):
        src = source_chip(*lay.offsets[i]) * C + core
        here(units.at[span(src, k)], pr.at[i, k]).wait_recv()

    def far_wait(i, g):
        src = source_chip(*lay.offsets[i]) * C + core
        k, count = pairs[g]
        here(units.at[span(src, k, count)], fr.at[i - len(lay.near), g]).wait_recv()

    def sibling_wait(i):
        src = chip if i < 0 else source_chip(*lay.offsets[i])
        part = units.at[span(src * C + lax.rem(core + 1, C), 0, chunks)]
        here(part, sr.at[i + 1]).wait_recv()

    sends_up = z < last
    sends_down = z == last
    relays_down = (z > 0) & (z < last - 1)

    def meets(src, dst):
        found = ((src < dst) & (dst < last)) | ((src == last - 1) & (dst == last))
        return found | ((src == last) & (dst < last - 1)) if lay.down else found

    def source(w):
        return last if w == 0 else z - w

    def valid(w):
        if w == 0:
            return z < last - 1
        found = (z >= w) & (z < last)
        return (found | (z == last)) if w == 1 else found

    def goes_on(w):
        return (z >= w) & (z < last - 1)

    def line_copy(src, k, dst_slot, tag, there):
        return remote(
            src, line.at[dst_slot, pl.ds(k * rows_here, rows_here)],
            ls.at[tag], lr.at[dst_slot, k], line_id(there),
        )

    def own_part(k):
        return units.at[span(slot, k)]

    def slot_part(w, k):
        return line.at[w, pl.ds(k * rows_here, rows_here)]

    def own_up(k):
        return line_copy(own_part(k), k, 1, 0, z + 1)

    def own_down(k):
        return line_copy(own_part(k), k, 0, 0, z - 2)

    def relay_up(w, k):
        return line_copy(slot_part(w, k), k, w + 1, 1 + w, z + 1)

    def relay_down(k):
        return line_copy(slot_part(0, k), k, 0, 1, z - 1)

    def line_wait(w, k):
        here(slot_part(w, k), lr.at[w, k]).wait_recv()

    def line_order(src, dst_slot, tag, there):
        return remote(src, line_orders.at[dst_slot], los.at[tag], lor.at[dst_slot], line_id(there))

    def order_up():
        return line_order(orders.at[slot], 1, 0, z + 1)

    def order_down():
        return line_order(orders.at[slot], 0, 0, z - 2)

    def order_on_up(w):
        return line_order(line_orders.at[w], w + 1, 1 + w, z + 1)

    def order_on_down():
        return line_order(line_orders.at[0], 0, 1, z - 1)

    def order_send(src, sem, where):
        return remote(orders.at[src], orders.at[src], os_, sem, where)

    def order_copy(i):
        return order_send(slot, or_.at[i], plane_id(*lay.offsets[i], 0))

    def order_relay(i):
        df, dx = lay.offsets[i]
        return order_send(source_chip(0, dx) * C + core, or_.at[i], plane_id(df, 0, 0))

    def order_wait(i):
        src = source_chip(*lay.offsets[i]) * C + core
        here(orders.at[src], or_.at[i]).wait_recv()

    def order_across(i):
        src = chip if i < 0 else source_chip(*lay.offsets[i])
        return order_send(src * C + core, osr.at[i + 1], plane_id(0, 0, 1))

    def order_across_wait(i):
        src = chip if i < 0 else source_chip(*lay.offsets[i])
        here(orders.at[src * C + lax.rem(core + 1, C)], osr.at[i + 1]).wait_recv()

    barrier = pltpu.get_barrier_semaphore()
    steps = [(*lay.offsets[i], 0) for i in lay.near] + ([(0, 0, 1)] if C > 1 else [])
    sides = ((z > 0, z - 1), (z < last, z + 1), (z == last - 2, z + 2))
    for step in steps:
        pl.semaphore_signal(barrier, inc=1, device_id=plane_id(*step), device_id_type=MESH)
    for there, which in sides:
        pl.when(there)(
            lambda which=which: pl.semaphore_signal(
                barrier, inc=1, device_id=line_id(which), device_id_type=MESH
            )
        )
    loads = [
        pltpu.make_async_copy(emb, raw, load.at[0]),
        pltpu.make_async_copy(order, own_order, load.at[1]),
    ]
    for one in loads:
        one.start()
    row_best[...] = jnp.full(row_best.shape, -1.0, jnp.float32)
    col_best[...] = jnp.full(col_best.shape, -1.0, jnp.float32)
    loads[1].wait()
    orders[pl.ds(slot, 1)] = own_order[...].reshape(1, 1, n)
    loads[0].wait()

    def normalize(k):
        floats = raw[pl.ds(k * rows_here, rows_here), :].astype(jnp.float32)
        scale = lax.rsqrt(jnp.sum(floats * floats, axis=1, keepdims=True) + 1e-06)
        units[span(slot, k), :] = (floats * scale).astype(jnp.bfloat16)

    for k in range(chunks):
        normalize(k)
    lines = jnp.minimum(z, 1) + jnp.minimum(last - z, 1)
    if lay.down:
        lines = lines + z // last
    pl.semaphore_wait(barrier, len(steps) + lines)

    def start(cond, *copies):
        @pl.when(cond)
        def run():
            for one in copies:
                one().start()

    early = (chunks + 2) // 3 if lay.hold else chunks
    holds = z == 1 if lay.hold else z < 0
    if S > 1:
        start(sends_up, order_up, *[functools.partial(own_up, k) for k in range(early)])
        start(sends_up & jnp.logical_not(holds),
              *[functools.partial(own_up, k) for k in range(early, chunks)])
    if lay.down:
        start(sends_down, order_down, *[functools.partial(own_down, k) for k in range(chunks)])
    for i in lay.near:
        order_copy(i).start()
    if C > 1:
        order_across(-1).start()
    for k in range(chunks):
        for i in lay.near:
            plane_copy(i, k).start()
        if C > 1 and k == 0:
            sibling_copy(-1, 0, chunks).start()

    def spread(which, row):
        wide = jnp.broadcast_to(row.reshape(1, n), (LANES, n))
        col_orders[which] = wide.T

    spread(own, orders[slot])

    width = C * n

    def scores(lhs, first_chip, wide=1):
        rhs = units[pl.ds(pl.multiple_of(first_chip * width, LANES), wide * width), :]
        return lax.dot_general(
            lhs, rhs, (((1,), (1,)), ((), ())), preferred_element_type=jnp.float32
        )

    def fold(s, w, first_chip, both, first=0, count=n, wide=1):
        mine = col_orders[w, first:first + count, :]
        rows_max = None
        for j in range(wide * width // LANES):
            part = s[:, j * LANES:(j + 1) * LANES]
            which_chip, at = first_chip + j * LANES // width, j * LANES % width
            core_at, lane_at = at // n, at % n
            theirs = orders[which_chip * C + core_at, :, lane_at:lane_at + LANES]
            earlier = theirs < mine
            if both:
                cand = jnp.where(earlier, part, jnp.float32(-1.0))
                rows_max = cand if rows_max is None else jnp.maximum(rows_max, cand)
                later = jnp.where(earlier, jnp.float32(-1.0), part)
            else:
                later = jnp.where(mine < theirs, part, jnp.float32(-1.0))
            down = jnp.max(later.reshape(count // 8, 8, LANES), axis=0)
            col_best[which_chip, :, at:at + LANES] = jnp.maximum(
                col_best[which_chip, :, at:at + LANES], down
            )
        if both:
            row_best[w, first:first + count, :] = jnp.maximum(
                row_best[w, first:first + count, :], rows_max
            )

    def own_rows():
        return units[pl.ds(pl.multiple_of(slot * n, LANES), n), :]

    def own_item(which_chip):
        fold(scores(own_rows(), which_chip), own, which_chip, False)

    def run_all(jobs):
        ready = None
        for w, first, count, one in jobs:
            lhs = own_rows() if w == own else line[w, first:first + count, :]
            s = scores(lhs, one)
            if ready is not None:
                fold(*ready)
            ready = (s, w, one, w != own, first, count)
        if ready is not None:
            fold(*ready)

    def chips_of(places):
        def at(j):
            if places == "near":
                by_x = j < X - 1
                df = jnp.where(by_x, 0, j - (X - 2))
                dx = jnp.where(by_x, j + 1, 0)
            elif places == "far":
                df, dx = 1 + j // max(X - 1, 1), 1 + lax.rem(j, max(X - 1, 1))
            else:
                df, dx = 0, 0
            return source_chip(df, dx)

        return {"near": F + X - 2, "far": (F - 1) * (X - 1), "self": 1}[places], at

    def sweep(places, rows):
        count, at = chips_of(places)

        def step(j, carry):
            run_all([(*one, at(j)) for one in rows])
            return carry

        if count <= 2:
            run_all([(*one, at(j)) for j in range(count) for one in rows])
        else:
            lax.fori_loop(0, count, step, 0)

    def line_sweep(w, places, first, count, cond):
        pl.when(valid(w) & cond)(lambda: sweep(places, [(w, first, count)]))

    def sweep_own(places):
        sweep(places, [(own, 0, n)])

    wide = next(m for m in (4, 3, 2, 1) if lay.chips % m == 0)

    def wide_sweep(w, first, count, cond):
        def body(j, carry):
            s = scores(line[w, first:first + count, :], j * wide, wide)
            fold(s, w, j * wide, True, first, count, wide)
            return carry

        @pl.when(valid(w) & cond)
        def run():
            lax.fori_loop(0, lay.chips // wide, body, 0)

    for i in lay.near:
        order_wait(i)
        if C > 1:
            order_across(i).start()
    for i in lay.far:
        order_relay(i).start()

    def take_order(w, cond):
        @pl.when(cond)
        def run():
            here(line_orders.at[w], lor.at[w]).wait_recv()
            if w == 0:
                pl.when(relays_down)(lambda: order_on_down().start())
            elif w < last - 1:
                pl.when(goes_on(w))(lambda: order_on_up(w).start())
            spread(w, line_orders[w])

    if S > 1:
        take_order(1, valid(1))
    if C > 1:
        order_across_wait(-1)
        sibling_wait(-1)
    own_item(chip)
    held = z == 2 if lay.hold else z < 0
    straight = jnp.logical_not(held)
    half = early * rows_here

    def take(w, k, cond):
        @pl.when(cond)
        def run():
            line_wait(w, k)
            if w < last - 1:
                pl.when(goes_on(w))(lambda: relay_up(w, k).start())

    def take_down(p):
        for there in range(S - 3, 0, -1):
            k = p - 1 - 2 * (S - 3 - there)
            if k == 0:
                take_order(0, z == there)
            if 0 <= k < chunks:
                @pl.when(z == there)
                def run(k=k):
                    line_wait(0, k)
                    relay_down(k).start()

    def far_group(g):
        for i in lay.far:
            far_wait(i, g)
            if C > 1:
                sibling_copy(i, *pairs[g]).start()

    def near_chunk(k):
        for i in lay.near:
            near_wait(i, k)
        for i in lay.far:
            relay_copy(i, k).start()
        if C > 1:
            for i in lay.near:
                sibling_copy(i, k, 1).start()

    for p in range(chunks + 2 * max(S - 4, 0) + 1):
        if p < chunks and S > 1:
            take(1, p, valid(1) if p < early else valid(1) & straight)
        for w in range(2, last - 1):
            k = p - 2 * (w - 1)
            if k == 0:
                take_order(w, goes_on(w))
            if 0 <= k < chunks:
                take(w, k, goes_on(w))
        if lay.hold and p == chunks - 1:
            start(holds, *[functools.partial(own_up, k) for k in range(early, chunks)])
        take_down(p)
        if p < chunks:
            near_chunk(p)
        if lay.hold and p == early + 1:
            line_sweep(1, "self", 0, half, held)
    if C > 1:
        for i in lay.near:
            order_across_wait(i)
            sibling_wait(i)
    sweep_own("near")
    for i in lay.far:
        order_wait(i)
        if C > 1:
            order_across(i).start()
    far_group(0)
    ends = z == last - 1
    bottom = z == 0

    def line_result(w):
        return remote(line_res.at[w], line_in.at[z], lrs.at[w], lrr.at[z], line_id(source(w)))

    def give_back(w, cond):
        @pl.when(valid(w) & cond)
        def run():
            line_res[w] = jnp.max(row_best[w].T, axis=0, keepdims=True)
            line_result(w).start()

    def take_rows(w, cond):
        @pl.when(valid(w) & cond)
        def run():
            for k in range(chunks):
                line_wait(w, k)
        take_order(w, valid(w) & cond)

    if S > 1:
        line_sweep(1, "self", 0, n, straight)
        if lay.hold:
            line_sweep(1, "near", 0, half, held)
    if lay.down:
        line_sweep(0, "self", 0, n, relays_down)
    for w in range(2, last):
        take_rows(w, ends)
        line_sweep(w, "self", 0, n, z < last)
    for g in range(1, len(pairs) - 1):
        far_group(g)
    if S > 1:
        line_sweep(1, "near", 0, n, straight)
    for w in range(2, last):
        line_sweep(w, "near", 0, n, z < last)
    for g in range(max(len(pairs) - 1, 1), len(pairs)):
        far_group(g)
    if lay.down:
        line_sweep(0, "near", 0, n, relays_down)
    if C > 1:
        for i in lay.far:
            order_across_wait(i)
            sibling_wait(i)
    if lay.hold:
        pl.when(held)(lambda: sweep("far", [(own, 0, n), (2, 0, n), (1, 0, half)]))
        pl.when(z == 1)(lambda: sweep("far", [(own, 0, n), (0, 0, n), (1, 0, n)]))
        pl.when(z == last)(lambda: sweep("far", [(own, 0, n), (1, 0, n)]))
        pl.when(bottom)(lambda: sweep_own("far"))
    else:
        sweep_own("far")
        for w in range(2, last):
            line_sweep(w, "far", 0, n, z < last)
        if lay.down:
            line_sweep(0, "far", 0, n, relays_down)
        if S > 1:
            line_sweep(1, "far", 0, n, straight)
    for w in range(2, last):
        give_back(w, z < last)
    if S > 1:
        give_back(1, straight)
    if lay.down:
        give_back(0, relays_down)
        take_rows(0, bottom)
        wide_sweep(0, 0, n, bottom)
        give_back(0, bottom)
    final = (chunks - 1) * rows_here
    tail = final // LANES * LANES
    if lay.hold:
        for k in range(early, chunks - 1):
            take(1, k, held)
        if chunks - 1 > early:
            wide_sweep(1, half, final - half, held)
        if tail:
            @pl.when(held)
            def run():
                line_res[1, :, :tail] = jnp.max(row_best[1, :tail, :].T, axis=0, keepdims=True)
        take(1, chunks - 1, held)

    def result_copy(df, dx, dc):
        there = (lax.rem(f + df, F) * X + lax.rem(x + dx, X)) * C + lax.rem(core + dc, C)
        o = (df * X + dx) * C + dc
        return remote(plane_res.at[there], plane_in.at[o], rs, rr, plane_id(df, dx, dc))

    def flush(df, dx):
        one = lax.rem(f + df, F) * X + lax.rem(x + dx, X)
        flat = jnp.max(col_best[one], axis=0, keepdims=True)
        for core_at in range(C):
            plane_res[one * C + core_at] = flat[:, core_at * n:(core_at + 1) * n]

    def flush_out(df, dx, first=0):
        flush(df, dx)
        for dc in range(first, C):
            result_copy(df, dx, dc).start()

    def finish():
        def step(j, carry):
            flush_out((lay.chips - 1 - j) // X, lax.rem(lay.chips - 1 - j, X))
            return carry

        if lay.chips > 4:
            lax.fori_loop(0, lay.chips - 1, step, 0)
        else:
            for j in range(lay.chips - 1, 0, -1):
                flush_out(j // X, j % X)
        flush_out(0, 0, 1)

    def finish_late():
        ready = None
        for j in range(lay.chips - 1, -1, -1):
            df, dx = j // X, j % X
            at = lax.rem(f + df, F) * X + lax.rem(x + dx, X)
            s = scores(line[1, final:, :], at)
            if ready is not None:
                fold(*ready[0], 1, ready[1], True, final, n - final)
                flush_out(*ready[2])
            ready = (s,), at, (df, dx)
        fold(*ready[0], 1, ready[1], True, final, n - final)
        line_res[1, :, tail:] = jnp.max(row_best[1, tail:, :].T, axis=0, keepdims=True)
        line_result(1).start()
        flush_out(0, 0, 1)

    if lay.hold and lay.chips <= 4:
        pl.when(held)(finish_late)
        pl.when(straight)(finish)
    elif lay.hold:
        wide_sweep(1, final, n - final, held)
        give_back(1, held)
        finish()
    else:
        finish()

    best = jnp.maximum(plane_res[slot], jnp.float32(-1.0))
    if lay.plane > 1:
        here(plane_in.at[pl.ds(1, lay.plane - 1)], rr).wait_recv()
        best = jnp.maximum(best, jnp.max(plane_in[1:], axis=0))
    plane_res[slot] = best
    for src in range(S):
        def gather(src=src):
            here(line_in.at[src], lrr.at[src]).wait_recv()
            plane_res[slot] = jnp.maximum(plane_res[slot], line_in[src])

        pl.when(meets(z, jnp.int32(src)))(gather)
    out[...] = plane_res[slot].reshape(n)

    def sent(part, sem):
        here(part, sem).wait_send()

    if lay.plane > 1:
        sent(units.at[pl.ds(0, (lay.plane - 1) * n)], ps)
        sent(orders.at[pl.ds(0, lay.plane - 1)], os_)
        sent(plane_in.at[pl.ds(1, lay.plane - 1)], rs)

    def line_sent(cond, tag):
        @pl.when(cond)
        def run():
            sent(line.at[0], ls.at[tag])
            sent(line_orders.at[0], los.at[tag])

    if S > 1:
        line_sent((sends_up | sends_down) if lay.down else sends_up, 0)
    if lay.down:
        line_sent(relays_down, 1)
    for w in range(1, last - 1):
        line_sent(goes_on(w), 1 + w)
    for w in range(S):
        if S > 1 and (w or lay.down):
            pl.when(valid(w))(lambda w=w: sent(line_res.at[w], lrs.at[w]))


def shards(lay, embeddings, doc_order):
    n, depth = embeddings.shape
    chunks = n // PIECE if n % PIECE == 0 else 1
    dma = pltpu.SemaphoreType.DMA
    S, near, far = lay.slow, max(len(lay.near), 1), max(len(lay.far), 1)
    vmem = pltpu.VMEM
    return pl.pallas_call(
        functools.partial(kernel, lay, n, chunks),
        out_shape=vmem((n,), jnp.float32),
        in_specs=[pl.BlockSpec(memory_space=pl.ANY)] * 2,
        out_specs=pl.BlockSpec(memory_space=vmem),
        scratch_shapes=[
            vmem((n, depth), jnp.bfloat16),
            vmem((n,), jnp.int32),
            vmem((lay.plane * n, depth), jnp.bfloat16),
            vmem((lay.slots, n, depth), jnp.bfloat16),
            vmem((lay.plane, 1, n), jnp.int32),
            vmem((lay.slots, 1, n), jnp.int32),
            vmem((lay.slots + 1, n, LANES), jnp.int32),
            vmem((lay.slots, n, LANES), jnp.float32),
            vmem((lay.chips, 8, lay.cores * n), jnp.float32),
            vmem((lay.plane, 1, n), jnp.float32),
            vmem((lay.slots, 1, n), jnp.float32),
            vmem((lay.plane, 1, n), jnp.float32),
            vmem((S, 1, n), jnp.float32),
            dma((2,)),
            dma(()), dma((near, chunks)), dma((far, (chunks + 1) // 2)), dma((near + far + 1,)),
            dma((S,)), dma((lay.slots, chunks)),
            dma(()), dma((near + far,)), dma((near + far + 1,)),
            dma((S,)), dma((lay.slots,)),
            dma(()), dma(()),
            dma((lay.slots,)), dma((S,)),
        ],
        compiler_params=pltpu.CompilerParams(
            collective_id=0, has_side_effects=True, vmem_limit_bytes=60 * 1024 * 1024
        ),
    )(embeddings, doc_order)


def solution(mesh):
    lay = Layout(mesh.shape["row"], mesh.shape["col"])
    return jax.shard_map(
        functools.partial(shards, lay),
        mesh=mesh,
        in_specs=(P(("row", "col"), None), P(("row", "col"))),
        out_specs=P(("row", "col")),
        check_vma=False,
    )
```

```python
import functools

import jax
import jax.numpy as jnp
from jax import lax
from jax.experimental import pallas as pl
from jax.experimental.pallas import tpu as pltpu
from jax.sharding import PartitionSpec as P

MESH = pl.DeviceIdType.MESH
LANES = 128
PIECE = 64


def fast_size(rows):
    best = 1
    for size in range(1, rows + 1):
        if rows % size == 0 and size * size <= rows:
            best = size
    return best


class Layout:
    def __init__(self, rows, cols):
        self.fast = fast_size(rows)
        self.slow = rows // self.fast
        self.cores = 2 if cols % 2 == 0 else 1
        self.xs = cols // self.cores
        self.chips = self.fast * self.xs
        self.plane = self.chips * self.cores
        self.down = self.slow > 2
        self.slots = max(self.slow - 2, 1) + 1
        self.hold = self.slow == 4
        chips = [(f, x) for f in range(self.fast) for x in range(self.xs)]
        near = [c for c in chips if (c[0] == 0) != (c[1] == 0)]
        far = [c for c in chips if c[0] != 0 and c[1] != 0]
        self.offsets = near + far
        self.near = list(range(len(near)))
        self.far = list(range(len(near), len(near) + len(far)))


def kernel(
    lay, n, chunks,
    emb, order, out,
    raw, own_order, units, line, orders, line_orders, col_orders,
    row_best, col_best, plane_res, line_res, plane_in, line_in,
    load, ps, pr, fr, sr, ls, lr, os_, or_, osr, los, lor, rs, rr, lrs, lrr,
):
    S, F, X, C = lay.slow, lay.fast, lay.xs, lay.cores
    own = lay.slots
    last = S - 1
    rows_here = n // chunks
    early = (chunks + 1) // 2 if lay.hold else chunks
    half = early * rows_here
    align = PIECE if rows_here % PIECE == 0 else rows_here
    r, c = lax.axis_index("row"), lax.axis_index("col")
    z, f = r // F, lax.rem(r, F)
    x, core = c // C, lax.rem(c, C)
    chip = f * X + x
    slot = chip * C + core

    def plane_id(df, dx, dc):
        return {
            "row": z * F + lax.rem(f + df, F),
            "col": lax.rem(x + dx, X) * C + lax.rem(core + dc, C),
        }

    def line_id(there):
        return {"row": there * F + f, "col": c}

    def source_chip(df, dx):
        return lax.rem(f + F - df, F) * X + lax.rem(x + X - dx, X)

    def span(which, k, count=1):
        return pl.ds(pl.multiple_of(which * n + k * rows_here, align), count * rows_here)

    def remote(src, dst, send, recv, where):
        return pltpu.make_async_remote_copy(
            src_ref=src, dst_ref=dst, send_sem=send, recv_sem=recv,
            device_id=where, device_id_type=MESH,
        )

    def here(part, sem):
        return remote(part, part, sem, sem, plane_id(0, 0, 1))

    pairs = [(k, min(2, chunks - k)) for k in range(0, chunks, 2)]

    group_sizes = (1, len(lay.near), len(lay.far))

    def kind(i):
        return 0 if i < 0 else 1 if i in lay.near else 2

    def plane_copy(i, k):
        part = units.at[span(slot, k)]
        return remote(part, part, ps, pr.at[i, k // 2], plane_id(*lay.offsets[i], 0))

    def relay_copy(i, k):
        df, dx = lay.offsets[i]
        src, step = ((0, dx), (df, 0)) if k % 2 == 0 else ((df, 0), (0, dx))
        part = units.at[span(source_chip(*src) * C + core, k)]
        return remote(part, part, ps, fr.at[i - len(lay.near), k // 2], plane_id(*step, 0))

    def sibling_copy(i, k, count):
        src = chip if i < 0 else source_chip(*lay.offsets[i])
        part = units.at[span(src * C + core, k, count)]
        return remote(part, part, ps, sr.at[kind(i)], plane_id(0, 0, 1))

    def near_wait(i, g):
        src = source_chip(*lay.offsets[i]) * C + core
        here(units.at[span(src, *pairs[g])], pr.at[i, g]).wait_recv()

    def far_wait(i, g):
        src = source_chip(*lay.offsets[i]) * C + core
        k, count = pairs[g]
        here(units.at[span(src, k, count)], fr.at[i - len(lay.near), g]).wait_recv()

    def sibling_wait(which):
        count = group_sizes[which]
        here(units.at[pl.ds(0, count * n)], sr.at[which]).wait_recv()

    sends_up = z < last
    sends_down = z == last
    relays_down = (z > 0) & (z < last - 1)

    def meets(src, dst):
        found = ((src < dst) & (dst < last)) | ((src == last - 1) & (dst == last))
        return found | ((src == last) & (dst < last - 1)) if lay.down else found

    def source(w):
        return last if w == 0 else z - w

    def valid(w):
        if w == 0:
            return z < last - 1
        found = (z >= w) & (z < last)
        return (found | (z == last)) if w == 1 else found

    def goes_on(w):
        return (z >= w) & (z < last - 1)

    def lr_at(w, k):
        return lr.at[w, 0] if w > 1 and w == last - 1 else lr.at[w, k]

    def line_copy(src, k, dst_slot, tag, there):
        return remote(
            src, line.at[dst_slot, pl.ds(k * rows_here, rows_here)],
            ls.at[tag], lr_at(dst_slot, k), line_id(there),
        )

    def own_part(k):
        return units.at[span(slot, k)]

    def slot_part(w, k):
        return line.at[w, pl.ds(k * rows_here, rows_here)]

    def own_up(k):
        return line_copy(own_part(k), k, 1, 0, z + 1)

    held_back = list(range(early, chunks))
    tail_lead = [(0, k) for k in held_back[1:2] if C > 1] + [(C - 1, k) for k in held_back]
    tail_rest = [(0, k) for k in held_back if k not in held_back[1:2]] if C > 1 else []

    def tail_up(which, k):
        part = units.at[span(chip * C + which, k)]
        where = {"row": (z + 1) * F + f, "col": x * C + which}
        return remote(
            part, line.at[1, pl.ds(k * rows_here, rows_here)], ls.at[S - 1], lr.at[1, k], where
        )

    def own_down(k):
        return line_copy(own_part(k), k, 0, 0, z - 2)

    def relay_up(w, k):
        return line_copy(slot_part(w, k), k, w + 1, 1 + w, z + 1)

    def relay_down(k):
        return line_copy(slot_part(0, k), k, 0, 1, z - 1)

    def line_wait(w, k):
        here(slot_part(w, k), lr_at(w, k)).wait_recv()

    def line_order(src, dst_slot, tag, there):
        return remote(src, line_orders.at[dst_slot], los.at[tag], lor.at[dst_slot], line_id(there))

    def order_up():
        return line_order(orders.at[slot], 1, 0, z + 1)

    def order_down():
        return line_order(orders.at[slot], 0, 0, z - 2)

    def order_on_up(w):
        return line_order(line_orders.at[w], w + 1, 1 + w, z + 1)

    def order_on_down():
        return line_order(line_orders.at[0], 0, 1, z - 1)

    def order_send(src, sem, where):
        return remote(orders.at[src], orders.at[src], os_, sem, where)

    def order_copy(i):
        return order_send(slot, or_.at[0], plane_id(*lay.offsets[i], 0))

    def order_relay(i):
        df, dx = lay.offsets[i]
        return order_send(source_chip(0, dx) * C + core, or_.at[1], plane_id(df, 0, 0))

    def order_wait(which):
        here(orders.at[pl.ds(0, group_sizes[which])], or_.at[which - 1]).wait_recv()

    def order_across(i):
        src = chip if i < 0 else source_chip(*lay.offsets[i])
        return order_send(src * C + core, osr.at[kind(i)], plane_id(0, 0, 1))

    def order_across_wait(which):
        here(orders.at[pl.ds(0, group_sizes[which])], osr.at[which]).wait_recv()

    barrier = pltpu.get_barrier_semaphore()
    steps = [(*lay.offsets[i], 0) for i in lay.near] + ([(0, 0, 1)] if C > 1 else [])
    sides = ((z > 0, z - 1), (z < last, z + 1), (z == last - 2, z + 2))
    for step in steps:
        pl.semaphore_signal(barrier, inc=1, device_id=plane_id(*step), device_id_type=MESH)
    for there, which in sides:
        pl.when(there)(
            lambda which=which: pl.semaphore_signal(
                barrier, inc=1, device_id=line_id(which), device_id_type=MESH
            )
        )
    loads = [pltpu.make_async_copy(order, own_order, load.at[0])]
    for at, count in ((0, half), (half, n - half)):
        if count:
            rows = pl.ds(at, count)
            loads.append(pltpu.make_async_copy(emb.at[rows], raw.at[rows], load.at[len(loads)]))
    for one in loads:
        one.start()
    row_best[...] = jnp.full(row_best.shape, -1.0, jnp.float32)
    col_best[...] = jnp.full(col_best.shape, -1.0, jnp.float32)
    loads[0].wait()
    orders[pl.ds(slot, 1)] = own_order[...].reshape(1, 1, n)
    loads[1].wait()

    def normalize(k):
        floats = raw[pl.ds(k * rows_here, rows_here), :].astype(jnp.float32)
        scale = lax.rsqrt(jnp.sum(floats * floats, axis=1, keepdims=True) + 1e-06)
        units[span(slot, k), :] = (floats * scale).astype(jnp.bfloat16)

    for k in range(early):
        normalize(k)
    lines = jnp.minimum(z, 1) + jnp.minimum(last - z, 1)
    if lay.down:
        lines = lines + z // last
    pl.semaphore_wait(barrier, len(steps) + lines)

    def start(cond, *copies):
        @pl.when(cond)
        def run():
            for one in copies:
                one().start()

    holds = z == 1 if lay.hold else z < 0
    lead = core == C - 1
    if S > 1:
        start(sends_up, order_up, *[functools.partial(own_up, k) for k in range(early)])
    if half < n:
        loads[2].wait()
        for k in range(early, chunks):
            normalize(k)
    if half < n and S > 1:
        start(sends_up & jnp.logical_not(holds),
              *[functools.partial(own_up, k) for k in range(early, chunks)])
    if lay.down:
        start(sends_down, order_down, *[functools.partial(own_down, k) for k in range(chunks)])
    for i in lay.near:
        order_copy(i).start()
    if C > 1:
        order_across(-1).start()
    for k in range(chunks):
        for i in lay.near:
            plane_copy(i, k).start()
        if C > 1 and k == 0:
            sibling_copy(-1, 0, chunks).start()

    def spread(which, row):
        wide = jnp.broadcast_to(row.reshape(1, n), (LANES, n))
        col_orders[which] = wide.T

    spread(own, orders[slot])

    width = C * n

    def scores(lhs, first_chip, wide=1):
        rhs = units[pl.ds(pl.multiple_of(first_chip * width, LANES), wide * width), :]
        return lax.dot_general(
            lhs, rhs, (((1,), (1,)), ((), ())), preferred_element_type=jnp.float32
        )

    def fold(s, w, first_chip, both, first=0, count=n, wide=1):
        mine = col_orders[w, first:first + count, :]
        rows_max = None
        for j in range(wide * width // LANES):
            part = s[:, j * LANES:(j + 1) * LANES]
            which_chip, at = first_chip + j * LANES // width, j * LANES % width
            core_at, lane_at = at // n, at % n
            theirs = orders[which_chip * C + core_at, :, lane_at:lane_at + LANES]
            earlier = theirs < mine
            if both:
                cand = jnp.where(earlier, part, jnp.float32(-1.0))
                rows_max = cand if rows_max is None else jnp.maximum(rows_max, cand)
                later = jnp.where(earlier, jnp.float32(-1.0), part)
            else:
                later = jnp.where(mine < theirs, part, jnp.float32(-1.0))
            down = jnp.max(later.reshape(count // 8, 8, LANES), axis=0)
            col_best[which_chip, :, at:at + LANES] = jnp.maximum(
                col_best[which_chip, :, at:at + LANES], down
            )
        if both:
            row_best[w, first:first + count, :] = jnp.maximum(
                row_best[w, first:first + count, :], rows_max
            )

    def own_rows():
        return units[pl.ds(pl.multiple_of(slot * n, LANES), n), :]

    def own_item(which_chip):
        fold(scores(own_rows(), which_chip), own, which_chip, False)

    def run_all(jobs):
        ready = None
        for w, first, count, one in jobs:
            lhs = own_rows() if w == own else line[w, first:first + count, :]
            s = scores(lhs, one)
            if ready is not None:
                fold(*ready)
            ready = (s, w, one, w != own, first, count)
        if ready is not None:
            fold(*ready)

    def chips_of(places):
        def at(j):
            if places == "near":
                by_x = j < X - 1
                df = jnp.where(by_x, 0, j - (X - 2))
                dx = jnp.where(by_x, j + 1, 0)
            elif places == "far":
                df, dx = 1 + j // max(X - 1, 1), 1 + lax.rem(j, max(X - 1, 1))
            else:
                df, dx = 0, 0
            return source_chip(df, dx)

        return {"near": F + X - 2, "far": (F - 1) * (X - 1), "self": 1}[places], at

    def sweep(places, rows):
        count, at = chips_of(places)

        def step(j, carry):
            run_all([(*one, at(j)) for one in rows])
            return carry

        if count <= 2:
            run_all([(*one, at(j)) for j in range(count) for one in rows])
        else:
            lax.fori_loop(0, count, step, 0)

    def line_sweep(w, places, first, count, cond):
        pl.when(valid(w) & cond)(lambda: sweep(places, [(w, first, count)]))

    def sweep_own(places):
        sweep(places, [(own, 0, n)])

    wide = next(m for m in (4, 3, 2, 1) if lay.chips % m == 0)

    def wide_sweep(w, first, count, cond):
        def body(j, carry):
            s = scores(line[w, first:first + count, :], j * wide, wide)
            fold(s, w, j * wide, True, first, count, wide)
            return carry

        @pl.when(valid(w) & cond)
        def run():
            lax.fori_loop(0, lay.chips // wide, body, 0)

    if lay.near:
        order_wait(1)
    if C > 1:
        for i in lay.near:
            order_across(i).start()
    for i in lay.far:
        order_relay(i).start()

    def take_order(w, cond):
        @pl.when(cond)
        def run():
            here(line_orders.at[w], lor.at[w]).wait_recv()
            if w == 0:
                pl.when(relays_down)(lambda: order_on_down().start())
            elif w < last - 1:
                pl.when(goes_on(w))(lambda: order_on_up(w).start())
            spread(w, line_orders[w])

    if S > 1:
        take_order(1, valid(1))
    if C > 1:
        order_across_wait(0)
        sibling_wait(0)
    own_item(chip)
    held = z == 2 if lay.hold else z < 0
    straight = jnp.logical_not(held)

    def take(w, k, cond):
        @pl.when(cond)
        def run():
            line_wait(w, k)
            if w < last - 1:
                pl.when(goes_on(w))(lambda: relay_up(w, k).start())

    def take_down(p):
        for there in range(S - 3, 0, -1):
            k = p - 1 - 2 * (S - 3 - there)
            if k == 0:
                take_order(0, z == there)
            if 0 <= k < chunks:
                @pl.when(z == there)
                def run(k=k):
                    line_wait(0, k)
                    relay_down(k).start()

    def far_group(g):
        for i in lay.far:
            far_wait(i, g)
            if C > 1:
                sibling_copy(i, *pairs[g]).start()

    def near_group(g):
        for i in lay.near:
            near_wait(i, g)
        for k in range(pairs[g][0], sum(pairs[g])):
            for i in lay.far:
                relay_copy(i, k).start()
        if C > 1:
            for i in lay.near:
                sibling_copy(i, *pairs[g]).start()

    for p in range(chunks + 2 * max(S - 4, 0) + 1):
        if p < chunks and S > 1:
            take(1, p, valid(1) if p < early else valid(1) & straight)
        for w in range(2, last - 1):
            k = p - 2 * (w - 1)
            if k == 0:
                take_order(w, goes_on(w))
            if 0 <= k < chunks:
                take(w, k, goes_on(w))
        if lay.hold and p == chunks - 1:
            start(holds & lead, *[functools.partial(tail_up, *one) for one in tail_lead])
            if tail_rest:
                start(holds & (core == 0), *[functools.partial(tail_up, *one) for one in tail_rest])
        take_down(p)
        if p < chunks and (p % 2 or p == chunks - 1):
            near_group(p // 2)
        if lay.hold and p == early + 1:
            line_sweep(1, "self", 0, half, held)
    if C > 1:
        if lay.near:
            order_across_wait(1)
            sibling_wait(1)
    sweep_own("near")
    if lay.far:
        order_wait(2)
    if C > 1:
        for i in lay.far:
            order_across(i).start()
    far_group(0)
    ends = z == last - 1
    bottom = z == 0

    def line_result(w):
        return remote(line_res.at[w], line_in.at[z], lrs.at[w], lrr.at[z], line_id(source(w)))

    def give_back(w, cond):
        @pl.when(valid(w) & cond)
        def run():
            line_res[w] = jnp.max(row_best[w].T, axis=0, keepdims=True)
            line_result(w).start()

    def take_rows(w, cond):
        @pl.when(valid(w) & cond)
        def run():
            if w > 1 and w == last - 1:
                here(line.at[w], lr_at(w, 0)).wait_recv()
            else:
                for k in range(chunks):
                    line_wait(w, k)
        take_order(w, valid(w) & cond)

    if S > 1:
        line_sweep(1, "self", 0, n, straight)
        if lay.hold:
            line_sweep(1, "near", 0, half, held)
    if lay.down:
        line_sweep(0, "self", 0, n, relays_down)
    for w in range(2, last):
        take_rows(w, ends)
        line_sweep(w, "self", 0, n, z < last)
    for g in range(1, len(pairs) - 1):
        far_group(g)
    if lay.down:
        take_rows(0, bottom)
        line_sweep(0, "self", 0, n, bottom)
    for g in range(max(len(pairs) - 1, 1), len(pairs)):
        far_group(g)
    if S > 1:
        line_sweep(1, "near", 0, n, straight)
    for w in range(2, last):
        line_sweep(w, "near", 0, n, z < last)
    if lay.down:
        line_sweep(0, "near", 0, n, valid(0))
    if C > 1:
        if lay.far:
            order_across_wait(2)
            sibling_wait(2)
    if lay.hold:
        pl.when(held)(lambda: sweep("far", [(own, 0, n), (2, 0, n), (1, 0, half)]))
        pl.when(z == 1)(lambda: sweep("far", [(own, 0, n), (0, 0, n), (1, 0, n)]))
        pl.when(z == last)(lambda: sweep("far", [(own, 0, n), (1, 0, n)]))
        pl.when(bottom)(lambda: sweep("far", [(own, 0, n), (0, 0, n)]))
    else:
        sweep_own("far")
        for w in range(2, last):
            line_sweep(w, "far", 0, n, z < last)
        if lay.down:
            line_sweep(0, "far", 0, n, valid(0))
        if S > 1:
            line_sweep(1, "far", 0, n, straight)
    for w in range(2, last):
        give_back(w, z < last)
    if S > 1:
        give_back(1, straight)
    if lay.down:
        give_back(0, valid(0))
    kept = early
    final = kept * rows_here
    tail = final // LANES * LANES
    if lay.hold:
        for k in range(early, kept):
            take(1, k, held)
        if kept > early:
            wide_sweep(1, half, final - half, held)
        if tail:
            @pl.when(held)
            def run():
                line_res[1, :, :tail] = jnp.max(row_best[1, :tail, :].T, axis=0, keepdims=True)
        for k in range(kept, chunks):
            take(1, k, held)

    def result_copy(df, dx, dc):
        there = (lax.rem(f + df, F) * X + lax.rem(x + dx, X)) * C + lax.rem(core + dc, C)
        o = (df * X + dx) * C + dc
        return remote(plane_res.at[there], plane_in.at[o], rs, rr, plane_id(df, dx, dc))

    def flush(df, dx):
        one = lax.rem(f + df, F) * X + lax.rem(x + dx, X)
        flat = jnp.max(col_best[one], axis=0, keepdims=True)
        for core_at in range(C):
            plane_res[one * C + core_at] = flat[:, core_at * n:(core_at + 1) * n]

    def flush_out(df, dx, first=0):
        flush(df, dx)
        for dc in range(first, C):
            result_copy(df, dx, dc).start()

    def finish():
        def step(j, carry):
            flush_out((lay.chips - 1 - j) // X, lax.rem(lay.chips - 1 - j, X))
            return carry

        if lay.chips > 4:
            lax.fori_loop(0, lay.chips - 1, step, 0)
        else:
            for j in range(lay.chips - 1, 0, -1):
                flush_out(j // X, j % X)
        flush_out(0, 0, 1)

    def finish_late():
        ready = None
        for j in range(lay.chips - 1, -1, -1):
            df, dx = j // X, j % X
            at = lax.rem(f + df, F) * X + lax.rem(x + dx, X)
            s = scores(line[1, final:, :], at)
            if ready is not None:
                fold(*ready[0], 1, ready[1], True, final, n - final)
                flush_out(*ready[2])
            ready = (s,), at, (df, dx)
        fold(*ready[0], 1, ready[1], True, final, n - final)
        line_res[1, :, tail:] = jnp.max(row_best[1, tail:, :].T, axis=0, keepdims=True)
        line_result(1).start()
        flush_out(0, 0, 1)

    if lay.hold and lay.chips <= 4:
        pl.when(held)(finish_late)
        pl.when(straight)(finish)
    elif lay.hold:
        wide_sweep(1, final, n - final, held)
        give_back(1, held)
        finish()
    else:
        finish()

    best = jnp.maximum(plane_res[slot], jnp.float32(-1.0))
    if lay.plane > 1:
        here(plane_in.at[pl.ds(1, lay.plane - 1)], rr).wait_recv()
        best = jnp.maximum(best, jnp.max(plane_in[1:], axis=0))
    plane_res[slot] = best
    for src in range(S):
        def gather(src=src):
            here(line_in.at[src], lrr.at[src]).wait_recv()
            plane_res[slot] = jnp.maximum(plane_res[slot], line_in[src])

        pl.when(meets(z, jnp.int32(src)))(gather)
    out[...] = plane_res[slot].reshape(n)

    def sent(part, sem):
        here(part, sem).wait_send()

    if lay.plane > 1:
        sent(units.at[pl.ds(0, (lay.plane - 1) * n)], ps)
        sent(orders.at[pl.ds(0, lay.plane - 1)], os_)
        sent(plane_in.at[pl.ds(1, lay.plane - 1)], rs)

    def line_sent(cond, tag):
        @pl.when(cond)
        def run():
            sent(line.at[0], ls.at[tag])
            sent(line_orders.at[0], los.at[tag])

    if S > 1:
        whole = ((sends_up | sends_down) if lay.down else sends_up) & jnp.logical_not(holds)
        line_sent(whole, 0)
    if lay.hold:
        @pl.when(holds)
        def run():
            sent(line.at[0, pl.ds(0, half)], ls.at[0])
            sent(line_orders.at[0], los.at[0])

        def tail_sent(cond, pieces):
            if pieces:
                part = units.at[pl.ds(0, len(pieces) * rows_here)]
                pl.when(holds & cond)(lambda: sent(part, ls.at[S - 1]))

        tail_sent(lead, tail_lead)
        tail_sent(core == 0, tail_rest)
    if lay.down:
        line_sent(relays_down, 1)
    for w in range(1, last - 1):
        line_sent(goes_on(w), 1 + w)
    for w in range(S):
        if S > 1 and (w or lay.down):
            pl.when(valid(w))(lambda w=w: sent(line_res.at[w], lrs.at[w]))


def shards(lay, embeddings, doc_order):
    n, depth = embeddings.shape
    chunks = n // PIECE if n % PIECE == 0 else 1
    dma = pltpu.SemaphoreType.DMA
    S, near, far = lay.slow, max(len(lay.near), 1), max(len(lay.far), 1)
    vmem = pltpu.VMEM
    return pl.pallas_call(
        functools.partial(kernel, lay, n, chunks),
        out_shape=vmem((n,), jnp.float32),
        in_specs=[pl.BlockSpec(memory_space=pl.ANY)] * 2,
        out_specs=pl.BlockSpec(memory_space=vmem),
        scratch_shapes=[
            vmem((n, depth), jnp.bfloat16),
            vmem((n,), jnp.int32),
            vmem((lay.plane * n, depth), jnp.bfloat16),
            vmem((lay.slots, n, depth), jnp.bfloat16),
            vmem((lay.plane, 1, n), jnp.int32),
            vmem((lay.slots, 1, n), jnp.int32),
            vmem((lay.slots + 1, n, LANES), jnp.int32),
            vmem((lay.slots, n, LANES), jnp.float32),
            vmem((lay.chips, 8, lay.cores * n), jnp.float32),
            vmem((lay.plane, 1, n), jnp.float32),
            vmem((lay.slots, 1, n), jnp.float32),
            vmem((lay.plane, 1, n), jnp.float32),
            vmem((S, 1, n), jnp.float32),
            dma((3,)),
            dma(()), dma((near, (chunks + 1) // 2)), dma((far, (chunks + 1) // 2)), dma((3,)),
            dma((S,)), dma((lay.slots, chunks)),
            dma(()), dma((2,)), dma((3,)),
            dma((max(S - 1, 1),)), dma((lay.slots,)),
            dma(()), dma(()),
            dma((lay.slots,)), dma((S,)),
        ],
        compiler_params=pltpu.CompilerParams(
            collective_id=0, has_side_effects=True, vmem_limit_bytes=60 * 1024 * 1024
        ),
    )(embeddings, doc_order)


def solution(mesh):
    lay = Layout(mesh.shape["row"], mesh.shape["col"])
    return jax.shard_map(
        functools.partial(shards, lay),
        mesh=mesh,
        in_specs=(P(("row", "col"), None), P(("row", "col"))),
        out_specs=P(("row", "col")),
        check_vma=False,
    )
```

```python
import functools

import jax
import jax.numpy as jnp
from jax import lax
from jax.experimental import pallas as pl
from jax.experimental.pallas import tpu as pltpu
from jax.sharding import PartitionSpec as P

MESH = pl.DeviceIdType.MESH
LANES = 128
PIECE = 64


def fast_size(rows):
    best = 1
    for size in range(1, rows + 1):
        if rows % size == 0 and size * size <= rows:
            best = size
    return best


class Layout:
    def __init__(self, rows, cols):
        self.fast = fast_size(rows)
        self.slow = rows // self.fast
        self.cores = 2 if cols % 2 == 0 else 1
        self.xs = cols // self.cores
        self.chips = self.fast * self.xs
        self.plane = self.chips * self.cores
        self.down = self.slow > 2
        self.slots = max(self.slow - 2, 1) + 1
        self.hold = self.slow == 4
        chips = [(f, x) for f in range(self.fast) for x in range(self.xs)]
        near = [c for c in chips if (c[0] == 0) != (c[1] == 0)]
        far = [c for c in chips if c[0] != 0 and c[1] != 0]
        self.offsets = near + far
        self.near = list(range(len(near)))
        self.far = list(range(len(near), len(near) + len(far)))


def kernel(
    lay, n, chunks,
    emb, order, out,
    raw, own_order, units, line, orders, line_orders, col_orders,
    sums, row_best, col_best, plane_res, line_res, plane_in, line_in,
    load, ps, pr, fr, sr, ls, lr, os_, or_, osr, los, lor, rs, rr, lrs, lrr,
):
    S, F, X, C = lay.slow, lay.fast, lay.xs, lay.cores
    own = lay.slots
    last = S - 1
    rows_here = n // chunks
    early = (chunks + 1) // 2 if lay.hold else chunks
    half = early * rows_here
    align = PIECE if rows_here % PIECE == 0 else rows_here
    r, c = lax.axis_index("row"), lax.axis_index("col")
    z, f = r // F, lax.rem(r, F)
    x, core = c // C, lax.rem(c, C)
    chip = f * X + x
    slot = chip * C + core

    def plane_id(df, dx, dc):
        return {
            "row": z * F + lax.rem(f + df, F),
            "col": lax.rem(x + dx, X) * C + lax.rem(core + dc, C),
        }

    def line_id(there):
        return {"row": there * F + f, "col": c}

    def source_chip(df, dx):
        return lax.rem(f + F - df, F) * X + lax.rem(x + X - dx, X)

    def span(which, k, count=1):
        return pl.ds(pl.multiple_of(which * n + k * rows_here, align), count * rows_here)

    def remote(src, dst, send, recv, where):
        return pltpu.make_async_remote_copy(
            src_ref=src, dst_ref=dst, send_sem=send, recv_sem=recv,
            device_id=where, device_id_type=MESH,
        )

    def here(part, sem):
        return remote(part, part, sem, sem, plane_id(0, 0, 1))

    pairs = [(k, min(2, chunks - k)) for k in range(0, chunks, 2)]

    group_sizes = (1, len(lay.near), len(lay.far))

    def kind(i):
        return 0 if i < 0 else 1 if i in lay.near else 2

    def plane_copy(i, k):
        part = units.at[span(slot, k)]
        return remote(part, part, ps, pr.at[k // 2], plane_id(*lay.offsets[i], 0))

    def relay_copy(i, k):
        df, dx = lay.offsets[i]
        src, step = ((0, dx), (df, 0)) if k % 2 == 0 else ((df, 0), (0, dx))
        part = units.at[span(source_chip(*src) * C + core, k)]
        return remote(part, part, ps, fr.at[k // 2], plane_id(*step, 0))

    def sibling_copy(i, k, count):
        src = chip if i < 0 else source_chip(*lay.offsets[i])
        part = units.at[span(src * C + core, k, count)]
        return remote(part, part, ps, sr.at[kind(i)], plane_id(0, 0, 1))

    def near_wait(g):
        part = units.at[pl.ds(0, len(lay.near) * pairs[g][1] * rows_here)]
        here(part, pr.at[g]).wait_recv()

    def far_wait(g):
        part = units.at[pl.ds(0, len(lay.far) * pairs[g][1] * rows_here)]
        here(part, fr.at[g]).wait_recv()

    def sibling_wait(which):
        count = group_sizes[which]
        here(units.at[pl.ds(0, count * n)], sr.at[which]).wait_recv()

    sends_up = z < last
    sends_down = z == last
    relays_down = (z > 0) & (z < last - 1)

    def source(w):
        return last if w == 0 else z - w

    def valid(w, z=z):
        if w == 0:
            return (z < last - 1) & lay.down
        found = (z >= w) & (z < last)
        return (found | (z == last)) if w == 1 else found

    def goes_on(w, z=z):
        return (z >= w) & (z < last - 1)

    def results_of(src):
        return [(src + w, w) for w in range(1, lay.slots) if src + w < S and valid(w, src + w)] + [
            (there, 0) for there in range(S - 2) if src == last
        ]

    def place_of(w):
        found = jnp.int32(0)
        for there in range(S):
            if valid(w, there):
                owner = last if w == 0 else there - w
                found = jnp.where(z == there, results_of(owner).index((there, w)), found)
        return found

    def lr_at(w, k):
        return lr.at[w * chunks + (k if w < 2 or w != last - 1 else 0)]

    def line_copy(src, k, dst_slot, there):
        return remote(
            src, line.at[dst_slot, pl.ds(k * rows_here, rows_here)],
            ls, lr_at(dst_slot, k), line_id(there),
        )

    def own_part(k):
        return units.at[span(slot, k)]

    def slot_part(w, k):
        return line.at[w, pl.ds(k * rows_here, rows_here)]

    def own_up(k):
        return line_copy(own_part(k), k, 1, z + 1)

    held_back = list(range(early, chunks))
    depth = units.shape[1]
    by = len(held_back)
    cut = depth // by if by and depth % (by * LANES) == 0 else 0

    def held_part(row, k):
        if cut:
            return pl.ds(row + half, n - half), pl.ds((k - early) * cut, cut)
        return pl.ds(row + k * rows_here, rows_here), slice(None)

    tail_lead = [(0, k) for k in held_back[1:2] if C > 1] + [(C - 1, k) for k in held_back]
    tail_rest = [(0, k) for k in held_back if k not in held_back[1:2]] if C > 1 else []

    def tail_up(which, k):
        row = pl.multiple_of((chip * C + which) * n, LANES)
        where = {"row": (z + 1) * F + f, "col": x * C + which}
        return remote(
            units.at[held_part(row, k)], line.at[(1, *held_part(0, k))], ls, lr_at(1, k), where
        )

    def own_down(k):
        return line_copy(own_part(k), k, 0, z - 2)

    def relay_up(w, k):
        return line_copy(slot_part(w, k), k, w + 1, z + 1)

    def relay_down(k):
        return line_copy(slot_part(0, k), k, 0, z - 1)

    def line_wait(w, k):
        here(slot_part(w, k), lr_at(w, k)).wait_recv()

    def line_order(src, dst_slot, there):
        return remote(src, line_orders.at[dst_slot], los, lor.at[dst_slot], line_id(there))

    def order_up():
        return line_order(orders.at[slot], 1, z + 1)

    def order_down():
        return line_order(orders.at[slot], 0, z - 2)

    def order_on_up(w):
        return line_order(line_orders.at[w], w + 1, z + 1)

    def order_on_down():
        return line_order(line_orders.at[0], 0, z - 1)

    def order_send(src, sem, where):
        return remote(orders.at[src], orders.at[src], os_, sem, where)

    def order_copy(i):
        return order_send(slot, or_.at[0], plane_id(*lay.offsets[i], 0))

    def order_relay(i):
        df, dx = lay.offsets[i]
        return order_send(source_chip(0, dx) * C + core, or_.at[1], plane_id(df, 0, 0))

    def order_wait(which):
        here(orders.at[pl.ds(0, group_sizes[which])], or_.at[which - 1]).wait_recv()

    def order_across(i):
        src = chip if i < 0 else source_chip(*lay.offsets[i])
        return order_send(src * C + core, osr.at[kind(i)], plane_id(0, 0, 1))

    def order_across_wait(which):
        here(orders.at[pl.ds(0, group_sizes[which])], osr.at[which]).wait_recv()

    barrier = pltpu.get_barrier_semaphore()
    steps = [(*lay.offsets[i], 0) for i in lay.near] + ([(0, 0, 1)] if C > 1 else [])
    sides = ((z > 0, z - 1), (z < last, z + 1), (z == last - 2, z + 2))
    for step in steps:
        pl.semaphore_signal(barrier, inc=1, device_id=plane_id(*step), device_id_type=MESH)
    for there, which in sides:
        pl.when(there)(
            lambda which=which: pl.semaphore_signal(
                barrier, inc=1, device_id=line_id(which), device_id_type=MESH
            )
        )
    loads = [pltpu.make_async_copy(order, own_order, load.at[0])]
    for at, count in ((0, half), (half, n - half)):
        if count:
            rows = pl.ds(at, count)
            loads.append(pltpu.make_async_copy(emb.at[rows], raw.at[rows], load.at[len(loads)]))
    for one in loads:
        one.start()
    row_best[...] = jnp.full(row_best.shape, -1.0, jnp.float32)
    col_best[...] = jnp.full(col_best.shape, -1.0, jnp.float32)
    loads[0].wait()
    orders[pl.ds(slot, 1)] = own_order[...].reshape(1, 1, n)
    loads[1].wait()

    def normalize(k):
        floats = raw[pl.ds(k * rows_here, rows_here), :].astype(jnp.float32)
        scale = lax.rsqrt(jnp.sum(floats * floats, axis=1, keepdims=True) + 1e-06)
        units[span(slot, k), :] = (floats * scale).astype(jnp.bfloat16)

    for k in range(early):
        normalize(k)
    lines = jnp.minimum(z, 1) + jnp.minimum(last - z, 1)
    if lay.down:
        lines = lines + z // last
    pl.semaphore_wait(barrier, len(steps) + lines)

    def start(cond, *copies):
        @pl.when(cond)
        def run():
            for one in copies:
                one().start()

    holds = z == 1 if lay.hold else z < 0
    lead = core == C - 1
    if S > 1:
        start(sends_up, order_up, *[functools.partial(own_up, k) for k in range(early)])
    if half < n:
        loads[2].wait()
        for k in range(early, chunks):
            normalize(k)
    if half < n and S > 1:
        start(sends_up & jnp.logical_not(holds),
              *[functools.partial(own_up, k) for k in range(early, chunks)])
    if lay.down:
        start(sends_down, order_down, *[functools.partial(own_down, k) for k in range(chunks)])
    for i in lay.near:
        order_copy(i).start()
    if C > 1:
        order_across(-1).start()
    for k in range(chunks):
        for i in lay.near:
            plane_copy(i, k).start()
        if C > 1 and k == 0:
            sibling_copy(-1, 0, chunks).start()

    def spread(which, row):
        wide = jnp.broadcast_to(row.reshape(1, n), (LANES, n))
        col_orders[which] = wide.T

    spread(own, orders[slot])

    width = C * n

    def scores(lhs, first_chip, wide=1, depths=slice(None)):
        at = pl.multiple_of(first_chip * width, LANES)
        rhs = units[pl.ds(at, wide * width), depths]
        return lax.dot_general(
            lhs, rhs, (((1,), (1,)), ((), ())), preferred_element_type=jnp.float32
        )

    def fold(s, w, first_chip, both, first=0, count=n):
        mine = col_orders[w, first:first + count, :]
        rows_max = None
        for j in range(s.shape[1] // LANES):
            part = s[:, j * LANES:(j + 1) * LANES]
            which_chip, at = first_chip + j * LANES // width, j * LANES % width
            core_at, lane_at = at // n, at % n
            theirs = orders[which_chip * C + core_at, :, lane_at:lane_at + LANES]
            earlier = theirs < mine
            if both:
                cand = jnp.where(earlier, part, jnp.float32(-1.0))
                rows_max = cand if rows_max is None else jnp.maximum(rows_max, cand)
                later = jnp.where(earlier, jnp.float32(-1.0), part)
            else:
                later = jnp.where(mine < theirs, part, jnp.float32(-1.0))
            down = jnp.max(later.reshape(count // 8, 8, LANES), axis=0)
            col_best[which_chip, :, at:at + LANES] = jnp.maximum(
                col_best[which_chip, :, at:at + LANES], down
            )
        if both:
            row_best[w, first:first + count, :] = jnp.maximum(
                row_best[w, first:first + count, :], rows_max
            )

    def own_rows():
        return units[pl.ds(pl.multiple_of(slot * n, LANES), n), :]

    def own_item(which_chip):
        fold(scores(own_rows(), which_chip), own, which_chip, False)

    def run_all(jobs):
        ready = None
        for w, first, count, one in jobs:
            lhs = own_rows() if w == own else line[w, first:first + count, :]
            s = scores(lhs, one)
            if ready is not None:
                fold(*ready)
            ready = (s, w, one, w != own, first, count)
        if ready is not None:
            fold(*ready)

    def chips_of(places):
        def at(j):
            if places == "near":
                by_x = j < X - 1
                df = jnp.where(by_x, 0, j - (X - 2))
                dx = jnp.where(by_x, j + 1, 0)
            elif places == "far":
                df, dx = 1 + j // max(X - 1, 1), 1 + lax.rem(j, max(X - 1, 1))
            else:
                df, dx = 0, 0
            return source_chip(df, dx)

        return {"near": F + X - 2, "far": (F - 1) * (X - 1), "self": 1}[places], at

    def sweep(places, rows):
        count, at = chips_of(places)

        def step(j, carry):
            run_all([(*one, at(j)) for one in rows])
            return carry

        if count <= 2:
            run_all([(*one, at(j)) for j in range(count) for one in rows])
        else:
            lax.fori_loop(0, count, step, 0)

    def line_sweep(w, places, first, count, cond):
        pl.when(valid(w) & cond)(lambda: sweep(places, [(w, first, count)]))

    def sweep_own(places):
        sweep(places, [(own, 0, n)])

    wide = next(m for m in (4, 3, 2, 1) if lay.chips % m == 0)

    def wide_sweep(w, first, count, cond):
        def body(j, carry):
            s = scores(line[w, first:first + count, :], j * wide, wide)
            fold(s, w, j * wide, True, first, count)
            return carry

        @pl.when(valid(w) & cond)
        def run():
            lax.fori_loop(0, lay.chips // wide, body, 0)

    if lay.near:
        order_wait(1)
    if C > 1:
        for i in lay.near:
            order_across(i).start()
    for i in lay.far:
        order_relay(i).start()

    def take_order(w, cond):
        @pl.when(cond)
        def run():
            here(line_orders.at[w], lor.at[w]).wait_recv()
            if w == 0:
                pl.when(relays_down)(lambda: order_on_down().start())
            elif w < last - 1:
                pl.when(goes_on(w))(lambda: order_on_up(w).start())
            spread(w, line_orders[w])

    if S > 1:
        take_order(1, valid(1))
    if C > 1:
        order_across_wait(0)
        sibling_wait(0)
    own_item(chip)
    held = z == 2 if lay.hold else z < 0
    straight = jnp.logical_not(held)

    def take(w, k, cond):
        @pl.when(cond)
        def run():
            line_wait(w, k)
            if w < last - 1:
                pl.when(goes_on(w))(lambda: relay_up(w, k).start())

    def take_down(p):
        for there in range(S - 3, 0, -1):
            k = p - 1 - 2 * (S - 3 - there)
            if k == 0:
                take_order(0, z == there)
            if 0 <= k < chunks:
                @pl.when(z == there)
                def run(k=k):
                    line_wait(0, k)
                    relay_down(k).start()

    def far_group(g):
        if lay.far:
            far_wait(g)
        if C > 1:
            for i in lay.far:
                sibling_copy(i, *pairs[g]).start()

    def near_group(g):
        if lay.near:
            near_wait(g)
        for k in range(pairs[g][0], sum(pairs[g])):
            for i in lay.far:
                relay_copy(i, k).start()
        if C > 1:
            for i in lay.near:
                sibling_copy(i, *pairs[g]).start()

    for p in range(chunks + 2 * max(S - 4, 0) + 1):
        if p < chunks and S > 1:
            take(1, p, valid(1) if p < early else valid(1) & straight)
        for w in range(2, last - 1):
            k = p - 2 * (w - 1)
            if k == 0:
                take_order(w, goes_on(w))
            if 0 <= k < chunks:
                take(w, k, goes_on(w))
        if lay.hold and p == chunks - 1:
            start(holds & lead, *[functools.partial(tail_up, *one) for one in tail_lead])
            if tail_rest:
                start(holds & (core == 0), *[functools.partial(tail_up, *one) for one in tail_rest])
        take_down(p)
        if p < chunks and (p % 2 or p == chunks - 1):
            near_group(p // 2)
        if lay.hold and p == early + 1:
            line_sweep(1, "self", 0, half, held)
    if C > 1:
        if lay.near:
            order_across_wait(1)
            sibling_wait(1)
    sweep_own("near")
    if lay.far:
        order_wait(2)
    if C > 1:
        for i in lay.far:
            order_across(i).start()
    far_group(0)
    ends = z == last - 1
    bottom = z == 0

    def line_result(w):
        return remote(line_res.at[w], line_in.at[place_of(w)], lrs, lrr, line_id(source(w)))

    def give_back(w, cond):
        @pl.when(valid(w) & cond)
        def run():
            line_res[w] = jnp.max(row_best[w].T, axis=0, keepdims=True)
            line_result(w).start()

    def take_rows(w, cond):
        @pl.when(valid(w) & cond)
        def run():
            if w > 1 and w == last - 1:
                here(line.at[w], lr_at(w, 0)).wait_recv()
            else:
                for k in range(chunks):
                    line_wait(w, k)
        take_order(w, valid(w) & cond)

    if S > 1:
        line_sweep(1, "self", 0, n, straight)
        if lay.hold:
            line_sweep(1, "near", 0, half, held)
    if lay.down:
        line_sweep(0, "self", 0, n, relays_down)
    for g in range(1, len(pairs) - 1):
        far_group(g)
    if lay.down:
        take_rows(0, bottom)
        line_sweep(0, "self", 0, n, bottom)
    for g in range(max(len(pairs) - 1, 1), len(pairs)):
        far_group(g)
    for w in range(2, last):
        take_rows(w, ends)
        line_sweep(w, "self", 0, n, z < last if not lay.hold else lead)
    if S > 1:
        line_sweep(1, "near", 0, n, straight)
    for w in range(2, last):
        line_sweep(w, "near", 0, n, z < last if not lay.hold else lead)
    if lay.down:
        line_sweep(0, "near", 0, n, valid(0))
    if C > 1:
        if lay.far:
            order_across_wait(2)
            sibling_wait(2)
    if lay.hold:
        line_sweep(2, "far", 0, n, lead)
        if C > 1:
            wide_sweep(2, 0, n, core == 0)
        give_back(2, z < last)
        pl.when(held)(lambda: sweep("far", [(own, 0, n), (1, 0, half)]))
        pl.when(z == 1)(lambda: sweep("far", [(own, 0, n), (0, 0, n), (1, 0, n)]))
        pl.when(z == last)(lambda: sweep("far", [(own, 0, n), (1, 0, n)]))
        pl.when(bottom)(lambda: sweep("far", [(own, 0, n), (0, 0, n)]))
    else:
        sweep_own("far")
        for w in range(2, last):
            line_sweep(w, "far", 0, n, z < last)
        if lay.down:
            line_sweep(0, "far", 0, n, valid(0))
        if S > 1:
            line_sweep(1, "far", 0, n, straight)
    for w in range(2, 2 if lay.hold else last):
        give_back(w, z < last)
    if S > 1:
        give_back(1, straight)
    if lay.down:
        give_back(0, valid(0))
    tail = half // LANES * LANES
    rest = slice((by - 1) * cut, None) if cut else slice(None)

    def take_held(k):
        @pl.when(held)
        def run():
            here(line.at[(1, *held_part(0, k))], lr_at(1, k)).wait_recv()

    def places():
        return [(j // X, j % X) for j in range(lay.chips - 1, -1, -1)]

    def chip_at(df, dx):
        return lax.rem(f + df, F) * X + lax.rem(x + dx, X)

    def begin_late(first, stop):
        depths = slice(first * cut, stop * cut)
        for j, place in enumerate(places()):
            s = scores(line[1, half:, depths], chip_at(*place), 1, depths)
            sums[j] = s + sums[j] if first else s

    if lay.hold:
        if tail:
            @pl.when(held)
            def run():
                line_res[1, :, :tail] = jnp.max(row_best[1, :tail, :].T, axis=0, keepdims=True)
        ahead = cut and lay.chips <= 4
        for k in held_back[:-1]:
            take_held(k)
            if ahead:
                pl.when(held & lead)(lambda k=k: begin_late(k - early, k - early + 1))
        if ahead and C > 1 and by > 1:
            pl.when(held & (core == 0))(lambda: begin_late(0, by - 1))
        take_held(held_back[-1])

    def result_copy(df, dx, dc):
        there = (lax.rem(f + df, F) * X + lax.rem(x + dx, X)) * C + lax.rem(core + dc, C)
        o = (df * X + dx) * C + dc
        return remote(plane_res.at[there], plane_in.at[o], rs, rr, plane_id(df, dx, dc))

    def flush(df, dx):
        one = lax.rem(f + df, F) * X + lax.rem(x + dx, X)
        flat = jnp.max(col_best[one], axis=0, keepdims=True)
        for core_at in range(C):
            plane_res[one * C + core_at] = flat[:, core_at * n:(core_at + 1) * n]

    def flush_out(df, dx, first=0):
        flush(df, dx)
        for dc in range(first, C):
            result_copy(df, dx, dc).start()

    def finish():
        def step(j, carry):
            flush_out((lay.chips - 1 - j) // X, lax.rem(lay.chips - 1 - j, X))
            return carry

        if lay.chips > 4:
            lax.fori_loop(0, lay.chips - 1, step, 0)
        else:
            for j in range(lay.chips - 1, 0, -1):
                flush_out(j // X, j % X)
        flush_out(0, 0, 1)

    def finish_late():
        ready = None

        def settle():
            s, at, place = ready
            fold(s, 1, at, True, half, n - half)
            if place != (0, 0):
                flush_out(*place)

        for j, place in enumerate(places()):
            s = scores(line[1, half:, rest], chip_at(*place), 1, rest)
            if cut:
                s = s + sums[j]
            if ready is not None:
                settle()
            ready = s, chip_at(*place), place
        settle()
        line_res[1, :, tail:] = jnp.max(row_best[1, tail:, :].T, axis=0, keepdims=True)
        line_result(1).start()
        flush_out(0, 0, 1)

    if lay.hold and lay.chips <= 4:
        pl.when(held)(finish_late)
        pl.when(straight)(finish)
    elif lay.hold:
        wide_sweep(1, half, n - half, held)
        give_back(1, held)
        finish()
    else:
        finish()

    best = jnp.maximum(plane_res[slot], jnp.float32(-1.0))
    if lay.plane > 1:
        here(plane_in.at[pl.ds(1, lay.plane - 1)], rr).wait_recv()
        best = jnp.maximum(best, jnp.max(plane_in[1:], axis=0))
    plane_res[slot] = best
    for there in range(S):
        count = len(results_of(there))
        if count:
            @pl.when(z == there)
            def run(count=count):
                part = line_in.at[pl.ds(0, count)]
                here(part, lrr).wait_recv()
                plane_res[slot] = jnp.maximum(plane_res[slot], jnp.max(part[...], axis=0))
    out[...] = plane_res[slot].reshape(n)

    def sent(part, sem):
        here(part, sem).wait_send()

    if lay.plane > 1:
        sent(units.at[pl.ds(0, (lay.plane - 1) * n)], ps)
        sent(orders.at[pl.ds(0, lay.plane - 1)], os_)
        sent(plane_in.at[pl.ds(1, lay.plane - 1)], rs)

    def line_sent(cond, pieces, copies, results):
        @pl.when(cond)
        def run():
            if pieces:
                sent(units.at[pl.ds(0, pieces * rows_here)], ls)
            if copies:
                sent(orders.at[pl.ds(0, copies)], los)
            if results:
                sent(plane_in.at[pl.ds(0, results)], lrs)

    for there in range(S):
        moved = sum(bool(goes_on(w, there)) for w in range(1, last - 1))
        moved += bool(lay.down and 0 < there < last - 1)
        owns = there < last or lay.down
        results = sum(bool(valid(w, there)) for w in range(lay.slots))
        if S == 1:
            continue
        if lay.hold and there == 1:
            for cond, held_pieces in ((lead, tail_lead), (jnp.logical_not(lead), tail_rest)):
                pieces = early + moved * chunks + len(held_pieces)
                line_sent((z == there) & cond, pieces, moved + owns, results)
        else:
            line_sent(z == there, (moved + owns) * chunks, moved + owns, results)


def shards(lay, embeddings, doc_order):
    n, depth = embeddings.shape
    chunks = n // PIECE if n % PIECE == 0 else 1
    dma = pltpu.SemaphoreType.DMA
    S = lay.slow
    pieces = chunks * (lay.slots - lay.hold) + lay.hold
    vmem = pltpu.VMEM
    return pl.pallas_call(
        functools.partial(kernel, lay, n, chunks),
        out_shape=vmem((n,), jnp.float32),
        in_specs=[pl.BlockSpec(memory_space=pl.ANY)] * 2,
        out_specs=pl.BlockSpec(memory_space=vmem),
        scratch_shapes=[
            vmem((n, depth), jnp.bfloat16),
            vmem((n,), jnp.int32),
            vmem((lay.plane * n, depth), jnp.bfloat16),
            vmem((lay.slots, n, depth), jnp.bfloat16),
            vmem((lay.plane, 1, n), jnp.int32),
            vmem((lay.slots, 1, n), jnp.int32),
            vmem((lay.slots + 1, n, LANES), jnp.int32),
            vmem((min(lay.chips, 4), n // 2, lay.cores * n), jnp.float32),
            vmem((lay.slots, n, LANES), jnp.float32),
            vmem((lay.chips, 8, lay.cores * n), jnp.float32),
            vmem((lay.plane, 1, n), jnp.float32),
            vmem((lay.slots, 1, n), jnp.float32),
            vmem((lay.plane, 1, n), jnp.float32),
            vmem((S, 1, n), jnp.float32),
            dma((3,)),
            dma(()), dma(((chunks + 1) // 2,)), dma(((chunks + 1) // 2,)), dma((3,)),
            dma(()), dma((pieces,)),
            dma(()), dma((2,)), dma((3,)),
            dma(()), dma((lay.slots,)),
            dma(()), dma(()),
            dma(()), dma(()),
        ],
        compiler_params=pltpu.CompilerParams(
            collective_id=0, has_side_effects=True, vmem_limit_bytes=60 * 1024 * 1024
        ),
    )(embeddings, doc_order)


def solution(mesh):
    lay = Layout(mesh.shape["row"], mesh.shape["col"])
    return jax.shard_map(
        functools.partial(shards, lay),
        mesh=mesh,
        in_specs=(P(("row", "col"), None), P(("row", "col"))),
        out_specs=P(("row", "col")),
        check_vma=False,
    )
```

```python
import functools

import jax
import jax.numpy as jnp
from jax import lax
from jax.experimental import pallas as pl
from jax.experimental.pallas import tpu as pltpu
from jax.sharding import PartitionSpec as P

MESH = pl.DeviceIdType.MESH
LANES = 128
PIECE = 64


def fast_size(rows):
    best = 1
    for size in range(1, rows + 1):
        if rows % size == 0 and size * size <= rows:
            best = size
    return best


class Layout:
    def __init__(self, rows, cols):
        self.fast = fast_size(rows)
        self.slow = rows // self.fast
        self.cores = 2 if cols % 2 == 0 else 1
        self.xs = cols // self.cores
        self.chips = self.fast * self.xs
        self.plane = self.chips * self.cores
        self.down = self.slow > 2
        self.slots = max(self.slow - 2, 1) + 1
        self.hold = self.slow == 4
        chips = [(f, x) for f in range(self.fast) for x in range(self.xs)]
        near = [c for c in chips if (c[0] == 0) != (c[1] == 0)]
        far = [c for c in chips if c[0] != 0 and c[1] != 0]
        self.offsets = near + far
        self.near = list(range(len(near)))
        self.far = list(range(len(near), len(near) + len(far)))


def kernel(
    lay, n, chunks,
    emb, order, out,
    raw, own_order, units, line, orders, line_orders, col_orders,
    sums, row_best, col_best, plane_res, line_res, plane_in, line_in,
    load, ps, pr, fr, sr, ls, lr, os_, or_, osr, los, lor, rs, rr, lrs, lrr,
):
    S, F, X, C = lay.slow, lay.fast, lay.xs, lay.cores
    own = lay.slots
    last = S - 1
    rows_here = n // chunks
    early = (chunks + 1) // 2 if lay.hold else chunks
    half = early * rows_here
    align = PIECE if rows_here % PIECE == 0 else rows_here
    r, c = lax.axis_index("row"), lax.axis_index("col")
    z, f = r // F, lax.rem(r, F)
    x, core = c // C, lax.rem(c, C)
    chip = f * X + x
    slot = chip * C + core

    def plane_id(df, dx, dc):
        return {
            "row": z * F + lax.rem(f + df, F),
            "col": lax.rem(x + dx, X) * C + lax.rem(core + dc, C),
        }

    def line_id(there):
        return {"row": there * F + f, "col": c}

    def source_chip(df, dx):
        return lax.rem(f + F - df, F) * X + lax.rem(x + X - dx, X)

    def span(which, k, count=1):
        return pl.ds(pl.multiple_of(which * n + k * rows_here, align), count * rows_here)

    def remote(src, dst, send, recv, where):
        return pltpu.make_async_remote_copy(
            src_ref=src, dst_ref=dst, send_sem=send, recv_sem=recv,
            device_id=where, device_id_type=MESH,
        )

    def here(part, sem):
        return remote(part, part, sem, sem, plane_id(0, 0, 1))

    pairs = [(k, min(2, chunks - k)) for k in range(0, chunks, 2)]

    group_sizes = (1, len(lay.near), len(lay.far))

    def kind(i):
        return 0 if i < 0 else 1 if i in lay.near else 2

    def plane_copy(i, k):
        part = units.at[span(slot, k)]
        return remote(part, part, ps, pr.at[k // 2], plane_id(*lay.offsets[i], 0))

    def relay_copy(i, k):
        df, dx = lay.offsets[i]
        src, step = ((0, dx), (df, 0)) if k % 2 == 0 else ((df, 0), (0, dx))
        part = units.at[span(source_chip(*src) * C + core, k)]
        return remote(part, part, ps, fr.at[k // 2], plane_id(*step, 0))

    def sibling_copy(i, k, count):
        src = chip if i < 0 else source_chip(*lay.offsets[i])
        part = units.at[span(src * C + core, k, count)]
        return remote(part, part, ps, sr.at[kind(i)], plane_id(0, 0, 1))

    def near_wait(g):
        part = units.at[pl.ds(0, len(lay.near) * pairs[g][1] * rows_here)]
        here(part, pr.at[g]).wait_recv()

    def far_wait(g):
        part = units.at[pl.ds(0, len(lay.far) * pairs[g][1] * rows_here)]
        here(part, fr.at[g]).wait_recv()

    def sibling_wait(which):
        count = group_sizes[which]
        here(units.at[pl.ds(0, count * n)], sr.at[which]).wait_recv()

    sends_up = z < last
    sends_down = z == last
    relays_down = (z > 0) & (z < last - 1)

    def source(w):
        return last if w == 0 else z - w

    def valid(w, z=z):
        if w == 0:
            return (z < last - 1) & lay.down
        found = (z >= w) & (z < last)
        return (found | (z == last)) if w == 1 else found

    def goes_on(w, z=z):
        return (z >= w) & (z < last - 1)

    def results_of(src):
        return [(src + w, w) for w in range(1, lay.slots) if src + w < S and valid(w, src + w)] + [
            (there, 0) for there in range(S - 2) if src == last
        ]

    def place_of(w):
        found = jnp.int32(0)
        for there in range(S):
            if valid(w, there):
                owner = last if w == 0 else there - w
                found = jnp.where(z == there, results_of(owner).index((there, w)), found)
        return found

    def lr_at(w, k):
        return lr.at[w * chunks + (k if w < 2 or w != last - 1 else 0)]

    def line_copy(src, k, dst_slot, there):
        return remote(
            src, line.at[dst_slot, pl.ds(k * rows_here, rows_here)],
            ls, lr_at(dst_slot, k), line_id(there),
        )

    def own_part(k):
        return units.at[span(slot, k)]

    def slot_part(w, k):
        return line.at[w, pl.ds(k * rows_here, rows_here)]

    def own_up(k):
        return line_copy(own_part(k), k, 1, z + 1)

    held_back = list(range(early, chunks))
    depth = units.shape[1]
    by = len(held_back)
    cut = depth // by if by and depth % (by * LANES) == 0 else 0

    def held_part(row, k):
        if cut:
            return pl.ds(row + half, n - half), pl.ds((k - early) * cut, cut)
        return pl.ds(row + k * rows_here, rows_here), slice(None)

    tail_lead = [(0, k) for k in held_back[1:2] if C > 1] + [(C - 1, k) for k in held_back]
    tail_rest = [(0, k) for k in held_back if k not in held_back[1:2]] if C > 1 else []

    def tail_up(which, k):
        row = pl.multiple_of((chip * C + which) * n, LANES)
        where = {"row": (z + 1) * F + f, "col": x * C + which}
        return remote(
            units.at[held_part(row, k)], line.at[(1, *held_part(0, k))], ls, lr_at(1, k), where
        )

    def own_down(k):
        return line_copy(own_part(k), k, 0, z - 2)

    def relay_up(w, k):
        return line_copy(slot_part(w, k), k, w + 1, z + 1)

    def relay_down(k):
        return line_copy(slot_part(0, k), k, 0, z - 1)

    def line_wait(w, k):
        here(slot_part(w, k), lr_at(w, k)).wait_recv()

    def line_order(src, dst_slot, there):
        return remote(src, line_orders.at[dst_slot], los, lor.at[dst_slot], line_id(there))

    def order_up():
        return line_order(orders.at[slot], 1, z + 1)

    def order_down():
        return line_order(orders.at[slot], 0, z - 2)

    def order_on_up(w):
        return line_order(line_orders.at[w], w + 1, z + 1)

    def order_on_down():
        return line_order(line_orders.at[0], 0, z - 1)

    def order_send(src, sem, where):
        return remote(orders.at[src], orders.at[src], os_, sem, where)

    def order_copy(i):
        return order_send(slot, or_.at[0], plane_id(*lay.offsets[i], 0))

    def order_relay(i):
        df, dx = lay.offsets[i]
        return order_send(source_chip(0, dx) * C + core, or_.at[1], plane_id(df, 0, 0))

    def order_wait(which):
        here(orders.at[pl.ds(0, group_sizes[which])], or_.at[which - 1]).wait_recv()

    def order_across(i):
        src = chip if i < 0 else source_chip(*lay.offsets[i])
        return order_send(src * C + core, osr.at[kind(i)], plane_id(0, 0, 1))

    def order_across_wait(which):
        here(orders.at[pl.ds(0, group_sizes[which])], osr.at[which]).wait_recv()

    barrier = pltpu.get_barrier_semaphore()
    steps = [(*lay.offsets[i], 0) for i in lay.near] + ([(0, 0, 1)] if C > 1 else [])
    sides = ((z > 0, z - 1), (z < last, z + 1), (z == last - 2, z + 2))
    for step in steps:
        pl.semaphore_signal(barrier, inc=1, device_id=plane_id(*step), device_id_type=MESH)
    for there, which in sides:
        pl.when(there)(
            lambda which=which: pl.semaphore_signal(
                barrier, inc=1, device_id=line_id(which), device_id_type=MESH
            )
        )
    loads = [pltpu.make_async_copy(order, own_order, load.at[0])]
    for at, count in ((0, half), (half, n - half)):
        if count:
            rows = pl.ds(at, count)
            loads.append(pltpu.make_async_copy(emb.at[rows], raw.at[rows], load.at[len(loads)]))
    for one in loads:
        one.start()
    row_best[...] = jnp.full(row_best.shape, -1.0, jnp.float32)
    col_best[...] = jnp.full(col_best.shape, -1.0, jnp.float32)
    loads[0].wait()
    orders[pl.ds(slot, 1)] = own_order[...].reshape(1, 1, n)
    loads[1].wait()

    def normalize(k):
        floats = raw[pl.ds(k * rows_here, rows_here), :].astype(jnp.float32)
        scale = lax.rsqrt(jnp.sum(floats * floats, axis=1, keepdims=True) + 1e-06)
        units[span(slot, k), :] = (floats * scale).astype(jnp.bfloat16)

    for k in range(early):
        normalize(k)
    lines = jnp.minimum(z, 1) + jnp.minimum(last - z, 1)
    if lay.down:
        lines = lines + z // last
    pl.semaphore_wait(barrier, len(steps) + lines)

    def start(cond, *copies):
        @pl.when(cond)
        def run():
            for one in copies:
                one().start()

    holds = z == 1 if lay.hold else z < 0
    lead = core == C - 1
    if S > 1:
        start(sends_up, order_up, *[functools.partial(own_up, k) for k in range(early)])
    if half < n:
        loads[2].wait()
        for k in range(early, chunks):
            normalize(k)
    if half < n and S > 1:
        start(sends_up & jnp.logical_not(holds),
              *[functools.partial(own_up, k) for k in range(early, chunks)])
    if lay.down:
        start(sends_down, order_down, *[functools.partial(own_down, k) for k in range(chunks)])
    for i in lay.near:
        order_copy(i).start()
    if C > 1:
        order_across(-1).start()
    for k in range(chunks):
        for i in lay.near:
            plane_copy(i, k).start()
        if C > 1 and k == 0:
            sibling_copy(-1, 0, chunks).start()

    def spread(which, row):
        wide = jnp.broadcast_to(row.reshape(1, n), (LANES, n))
        col_orders[which] = wide.T

    spread(own, orders[slot])

    width = C * n

    def scores(lhs, first_chip, wide=1, depths=slice(None)):
        at = pl.multiple_of(first_chip * width, LANES)
        rhs = units[pl.ds(at, wide * width), depths]
        return lax.dot_general(
            lhs, rhs, (((1,), (1,)), ((), ())), preferred_element_type=jnp.float32
        )

    def fold(s, w, first_chip, both, first=0, count=n):
        mine = col_orders[w, first:first + count, :]
        rows_max = None
        for j in range(s.shape[1] // LANES):
            part = s[:, j * LANES:(j + 1) * LANES]
            which_chip, at = first_chip + j * LANES // width, j * LANES % width
            core_at, lane_at = at // n, at % n
            theirs = orders[which_chip * C + core_at, :, lane_at:lane_at + LANES]
            earlier = theirs < mine
            if both:
                cand = jnp.where(earlier, part, jnp.float32(-1.0))
                rows_max = cand if rows_max is None else jnp.maximum(rows_max, cand)
                later = jnp.where(earlier, jnp.float32(-1.0), part)
            else:
                later = jnp.where(mine < theirs, part, jnp.float32(-1.0))
            down = jnp.max(later.reshape(count // 8, 8, LANES), axis=0)
            col_best[which_chip, :, at:at + LANES] = jnp.maximum(
                col_best[which_chip, :, at:at + LANES], down
            )
        if both:
            row_best[w, first:first + count, :] = jnp.maximum(
                row_best[w, first:first + count, :], rows_max
            )

    def own_rows():
        return units[pl.ds(pl.multiple_of(slot * n, LANES), n), :]

    def own_item(which_chip):
        fold(scores(own_rows(), which_chip), own, which_chip, False)

    def run_all(jobs):
        ready = None
        for w, first, count, one in jobs:
            lhs = own_rows() if w == own else line[w, first:first + count, :]
            s = scores(lhs, one)
            if ready is not None:
                fold(*ready)
            ready = (s, w, one, w != own, first, count)
        if ready is not None:
            fold(*ready)

    def chips_of(places):
        def at(j):
            if places == "near":
                by_x = j < X - 1
                df = jnp.where(by_x, 0, j - (X - 2))
                dx = jnp.where(by_x, j + 1, 0)
            elif places == "far":
                df, dx = 1 + j // max(X - 1, 1), 1 + lax.rem(j, max(X - 1, 1))
            else:
                df, dx = 0, 0
            return source_chip(df, dx)

        return {"near": F + X - 2, "far": (F - 1) * (X - 1), "self": 1}[places], at

    def sweep(places, rows):
        count, at = chips_of(places)

        def step(j, carry):
            run_all([(*one, at(j)) for one in rows])
            return carry

        if count <= 2:
            run_all([(*one, at(j)) for j in range(count) for one in rows])
        else:
            lax.fori_loop(0, count, step, 0)

    def line_sweep(w, places, first, count, cond):
        pl.when(valid(w) & cond)(lambda: sweep(places, [(w, first, count)]))

    def sweep_own(places):
        sweep(places, [(own, 0, n)])

    wide = next(m for m in (4, 3, 2, 1) if lay.chips % m == 0)

    def wide_sweep(w, first, count, cond):
        def body(j, carry):
            s = scores(line[w, first:first + count, :], j * wide, wide)
            fold(s, w, j * wide, True, first, count)
            return carry

        @pl.when(valid(w) & cond)
        def run():
            lax.fori_loop(0, lay.chips // wide, body, 0)

    if lay.near:
        order_wait(1)
    if C > 1:
        for i in lay.near:
            order_across(i).start()
    for i in lay.far:
        order_relay(i).start()

    def take_order(w, cond):
        @pl.when(cond)
        def run():
            here(line_orders.at[w], lor.at[w]).wait_recv()
            if w == 0:
                pl.when(relays_down)(lambda: order_on_down().start())
            elif w < last - 1:
                pl.when(goes_on(w))(lambda: order_on_up(w).start())
            spread(w, line_orders[w])

    if S > 1:
        take_order(1, valid(1))
    if C > 1:
        order_across_wait(0)
        sibling_wait(0)
    own_item(chip)
    held = z == 2 if lay.hold else z < 0
    straight = jnp.logical_not(held)

    def take(w, k, cond):
        @pl.when(cond)
        def run():
            line_wait(w, k)
            if w < last - 1:
                pl.when(goes_on(w))(lambda: relay_up(w, k).start())

    def take_down(p):
        for there in range(S - 3, 0, -1):
            k = p - 1 - 2 * (S - 3 - there)
            if k == 0:
                take_order(0, z == there)
            if 0 <= k < chunks:
                @pl.when(z == there)
                def run(k=k):
                    line_wait(0, k)
                    relay_down(k).start()

    def far_group(g):
        if lay.far:
            far_wait(g)
        if C > 1:
            for i in lay.far:
                sibling_copy(i, *pairs[g]).start()

    def near_group(g):
        if lay.near:
            near_wait(g)
        for k in range(pairs[g][0], sum(pairs[g])):
            for i in lay.far:
                relay_copy(i, k).start()
        if C > 1:
            for i in lay.near:
                sibling_copy(i, *pairs[g]).start()

    for p in range(chunks + 2 * max(S - 4, 0) + 1):
        if p < chunks and S > 1:
            take(1, p, valid(1) if p < early else valid(1) & straight)
        for w in range(2, last - 1):
            k = p - 2 * (w - 1)
            if k == 0:
                take_order(w, goes_on(w))
            if 0 <= k < chunks:
                take(w, k, goes_on(w))
        if lay.hold and p == chunks - 1:
            if tail_rest:
                start(holds & (core == 0), *[functools.partial(tail_up, *one) for one in tail_rest])
        take_down(p)
        if p < chunks and (p % 2 or p == chunks - 1):
            near_group(p // 2)
        if lay.hold and p == early + 1:
            line_sweep(1, "self", 0, half, held)
    if C > 1:
        if lay.near:
            order_across_wait(1)
            sibling_wait(1)
    sweep_own("near")
    if lay.far:
        order_wait(2)
    if C > 1:
        for i in lay.far:
            order_across(i).start()
    far_group(0)
    ends = z == last - 1
    bottom = z == 0

    def line_result(w):
        return remote(line_res.at[w], line_in.at[place_of(w)], lrs, lrr, line_id(source(w)))

    def give_back(w, cond):
        @pl.when(valid(w) & cond)
        def run():
            line_res[w] = jnp.max(row_best[w].T, axis=0, keepdims=True)
            line_result(w).start()

    def take_rows(w, cond):
        @pl.when(valid(w) & cond)
        def run():
            if w > 1 and w == last - 1:
                here(line.at[w], lr_at(w, 0)).wait_recv()
            else:
                for k in range(chunks):
                    line_wait(w, k)
        take_order(w, valid(w) & cond)

    if lay.hold:
        start(holds & lead, *[functools.partial(tail_up, *one) for one in tail_lead])
    if S > 1:
        line_sweep(1, "self", 0, n, straight)
        if lay.hold:
            line_sweep(1, "near", 0, half, held)
    if lay.down:
        line_sweep(0, "self", 0, n, relays_down)
    for g in range(1, len(pairs) - 1):
        far_group(g)
    if lay.down:
        take_rows(0, bottom)
        line_sweep(0, "self", 0, n, bottom)
    for g in range(max(len(pairs) - 1, 1), len(pairs)):
        far_group(g)
    for w in range(2, last):
        take_rows(w, ends)
        line_sweep(w, "self", 0, n, z < last if not lay.hold else lead)
    if S > 1:
        line_sweep(1, "near", 0, n, straight)
    for w in range(2, last):
        line_sweep(w, "near", 0, n, z < last if not lay.hold else lead)
    if lay.down:
        line_sweep(0, "near", 0, n, valid(0))
    if C > 1:
        if lay.far:
            order_across_wait(2)
            sibling_wait(2)
    if lay.hold:
        line_sweep(2, "far", 0, n, lead)
        if C > 1:
            wide_sweep(2, 0, n, core == 0)
        give_back(2, z < last)
        pl.when(held)(lambda: sweep("far", [(own, 0, n), (1, 0, half)]))
        pl.when(z == 1)(lambda: sweep("far", [(own, 0, n), (0, 0, n), (1, 0, n)]))
        pl.when(z == last)(lambda: sweep("far", [(own, 0, n), (1, 0, n)]))
        pl.when(bottom)(lambda: sweep("far", [(own, 0, n), (0, 0, n)]))
    else:
        sweep_own("far")
        for w in range(2, last):
            line_sweep(w, "far", 0, n, z < last)
        if lay.down:
            line_sweep(0, "far", 0, n, valid(0))
        if S > 1:
            line_sweep(1, "far", 0, n, straight)
    for w in range(2, 2 if lay.hold else last):
        give_back(w, z < last)
    if S > 1:
        give_back(1, straight)
    if lay.down:
        give_back(0, valid(0))
    tail = half // LANES * LANES
    rest = slice((by - 1) * cut, None) if cut else slice(None)

    def take_held(k):
        @pl.when(held)
        def run():
            here(line.at[(1, *held_part(0, k))], lr_at(1, k)).wait_recv()

    def places():
        return [(j // X, j % X) for j in range(lay.chips - 1, -1, -1)]

    def chip_at(df, dx):
        return lax.rem(f + df, F) * X + lax.rem(x + dx, X)

    def begin_late(first, stop):
        depths = slice(first * cut, stop * cut)
        for j, place in enumerate(places()):
            s = scores(line[1, half:, depths], chip_at(*place), 1, depths)
            sums[j] = s + sums[j] if first else s

    if lay.hold:
        if tail:
            @pl.when(held)
            def run():
                line_res[1, :, :tail] = jnp.max(row_best[1, :tail, :].T, axis=0, keepdims=True)
        ahead = cut and lay.chips <= 4
        for k in held_back[:-1]:
            take_held(k)
            if ahead:
                pl.when(held & lead)(lambda k=k: begin_late(k - early, k - early + 1))
        if ahead and C > 1 and by > 1:
            pl.when(held & (core == 0))(lambda: begin_late(0, by - 1))
        take_held(held_back[-1])

    def result_copy(df, dx, dc):
        there = (lax.rem(f + df, F) * X + lax.rem(x + dx, X)) * C + lax.rem(core + dc, C)
        o = (df * X + dx) * C + dc
        return remote(plane_res.at[there], plane_in.at[o], rs, rr, plane_id(df, dx, dc))

    def flush(df, dx):
        one = lax.rem(f + df, F) * X + lax.rem(x + dx, X)
        flat = jnp.max(col_best[one], axis=0, keepdims=True)
        for core_at in range(C):
            plane_res[one * C + core_at] = flat[:, core_at * n:(core_at + 1) * n]

    def flush_out(df, dx, first=0):
        flush(df, dx)
        for dc in range(first, C):
            result_copy(df, dx, dc).start()

    def finish():
        def step(j, carry):
            flush_out((lay.chips - 1 - j) // X, lax.rem(lay.chips - 1 - j, X))
            return carry

        if lay.chips > 4:
            lax.fori_loop(0, lay.chips - 1, step, 0)
        else:
            for j in range(lay.chips - 1, 0, -1):
                flush_out(j // X, j % X)
        flush_out(0, 0, 1)

    def finish_late():
        ready = None

        def settle():
            s, at, place = ready
            fold(s, 1, at, True, half, n - half)
            if place != (0, 0):
                flush_out(*place)

        for j, place in enumerate(places()):
            s = scores(line[1, half:, rest], chip_at(*place), 1, rest)
            if cut:
                s = s + sums[j]
            if ready is not None:
                settle()
            ready = s, chip_at(*place), place
        settle()
        line_res[1, :, tail:] = jnp.max(row_best[1, tail:, :].T, axis=0, keepdims=True)
        line_result(1).start()
        flush_out(0, 0, 1)

    if lay.hold and lay.chips <= 4:
        pl.when(held)(finish_late)
        pl.when(straight)(finish)
    elif lay.hold:
        wide_sweep(1, half, n - half, held)
        give_back(1, held)
        finish()
    else:
        finish()

    best = jnp.maximum(plane_res[slot], jnp.float32(-1.0))
    if lay.plane > 1:
        here(plane_in.at[pl.ds(1, lay.plane - 1)], rr).wait_recv()
        best = jnp.maximum(best, jnp.max(plane_in[1:], axis=0))
    plane_res[slot] = best
    for there in range(S):
        count = len(results_of(there))
        if count:
            @pl.when(z == there)
            def run(count=count):
                part = line_in.at[pl.ds(0, count)]
                here(part, lrr).wait_recv()
                plane_res[slot] = jnp.maximum(plane_res[slot], jnp.max(part[...], axis=0))
    out[...] = plane_res[slot].reshape(n)

    def sent(part, sem):
        here(part, sem).wait_send()

    if lay.plane > 1:
        sent(units.at[pl.ds(0, (lay.plane - 1) * n)], ps)
        sent(orders.at[pl.ds(0, lay.plane - 1)], os_)
        sent(plane_in.at[pl.ds(1, lay.plane - 1)], rs)

    def line_sent(cond, pieces, copies, results):
        @pl.when(cond)
        def run():
            if pieces:
                sent(units.at[pl.ds(0, pieces * rows_here)], ls)
            if copies:
                sent(orders.at[pl.ds(0, copies)], los)
            if results:
                sent(plane_in.at[pl.ds(0, results)], lrs)

    for there in range(S):
        moved = sum(bool(goes_on(w, there)) for w in range(1, last - 1))
        moved += bool(lay.down and 0 < there < last - 1)
        owns = there < last or lay.down
        results = sum(bool(valid(w, there)) for w in range(lay.slots))
        if S == 1:
            continue
        if lay.hold and there == 1:
            for cond, held_pieces in ((lead, tail_lead), (jnp.logical_not(lead), tail_rest)):
                pieces = early + moved * chunks + len(held_pieces)
                line_sent((z == there) & cond, pieces, moved + owns, results)
        else:
            line_sent(z == there, (moved + owns) * chunks, moved + owns, results)


def shards(lay, embeddings, doc_order):
    n, depth = embeddings.shape
    chunks = n // PIECE if n % PIECE == 0 else 1
    dma = pltpu.SemaphoreType.DMA
    S = lay.slow
    pieces = chunks * (lay.slots - lay.hold) + lay.hold
    vmem = pltpu.VMEM
    return pl.pallas_call(
        functools.partial(kernel, lay, n, chunks),
        out_shape=vmem((n,), jnp.float32),
        in_specs=[pl.BlockSpec(memory_space=pl.ANY)] * 2,
        out_specs=pl.BlockSpec(memory_space=vmem),
        scratch_shapes=[
            vmem((n, depth), jnp.bfloat16),
            vmem((n,), jnp.int32),
            vmem((lay.plane * n, depth), jnp.bfloat16),
            vmem((lay.slots, n, depth), jnp.bfloat16),
            vmem((lay.plane, 1, n), jnp.int32),
            vmem((lay.slots, 1, n), jnp.int32),
            vmem((lay.slots + 1, n, LANES), jnp.int32),
            vmem((min(lay.chips, 4), n // 2, lay.cores * n), jnp.float32),
            vmem((lay.slots, n, LANES), jnp.float32),
            vmem((lay.chips, 8, lay.cores * n), jnp.float32),
            vmem((lay.plane, 1, n), jnp.float32),
            vmem((lay.slots, 1, n), jnp.float32),
            vmem((lay.plane, 1, n), jnp.float32),
            vmem((S, 1, n), jnp.float32),
            dma((3,)),
            dma(()), dma(((chunks + 1) // 2,)), dma(((chunks + 1) // 2,)), dma((3,)),
            dma(()), dma((pieces,)),
            dma(()), dma((2,)), dma((3,)),
            dma(()), dma((lay.slots,)),
            dma(()), dma(()),
            dma(()), dma(()),
        ],
        compiler_params=pltpu.CompilerParams(
            collective_id=0, has_side_effects=True, vmem_limit_bytes=60 * 1024 * 1024
        ),
    )(embeddings, doc_order)


def solution(mesh):
    lay = Layout(mesh.shape["row"], mesh.shape["col"])
    return jax.shard_map(
        functools.partial(shards, lay),
        mesh=mesh,
        in_specs=(P(("row", "col"), None), P(("row", "col"))),
        out_specs=P(("row", "col")),
        check_vma=False,
    )
```

```python
import functools

import jax
import jax.numpy as jnp
from jax import lax
from jax.experimental import pallas as pl
from jax.experimental.pallas import tpu as pltpu
from jax.sharding import PartitionSpec as P

MESH = pl.DeviceIdType.MESH
LANES = 128
PIECE = 64


def fast_size(rows):
    best = 1
    for size in range(1, rows + 1):
        if rows % size == 0 and size * size <= rows:
            best = size
    return best


class Layout:
    def __init__(self, rows, cols):
        self.fast = fast_size(rows)
        self.slow = rows // self.fast
        self.cores = 2 if cols % 2 == 0 else 1
        self.xs = cols // self.cores
        self.chips = self.fast * self.xs
        self.plane = self.chips * self.cores
        self.down = self.slow > 2
        self.slots = max(self.slow - 2, 1) + 1
        self.hold = self.slow == 4
        chips = [(f, x) for f in range(self.fast) for x in range(self.xs)]
        near = [c for c in chips if (c[0] == 0) != (c[1] == 0)]
        far = [c for c in chips if c[0] != 0 and c[1] != 0]
        self.offsets = near + far
        self.near = list(range(len(near)))
        self.far = list(range(len(near), len(near) + len(far)))


def kernel(
    lay, n, chunks,
    emb, order, out,
    raw, own_order, units, line, orders, line_orders, col_orders,
    sums, row_best, col_best, plane_res, line_res, plane_in, line_in,
    load, ps, pr, fr, sr, ls, lr, os_, or_, osr, los, lor, rs, rr, lrs, lrr,
):
    S, F, X, C = lay.slow, lay.fast, lay.xs, lay.cores
    own = lay.slots
    last = S - 1
    rows_here = n // chunks
    early = (chunks + 1) // 2 if lay.hold else chunks
    half = early * rows_here
    align = PIECE if rows_here % PIECE == 0 else rows_here
    r, c = lax.axis_index("row"), lax.axis_index("col")
    z, f = r // F, lax.rem(r, F)
    x, core = c // C, lax.rem(c, C)
    chip = f * X + x
    slot = chip * C + core

    def plane_id(df, dx, dc):
        return {
            "row": z * F + lax.rem(f + df, F),
            "col": lax.rem(x + dx, X) * C + lax.rem(core + dc, C),
        }

    def line_id(there):
        return {"row": there * F + f, "col": c}

    def source_chip(df, dx):
        return lax.rem(f + F - df, F) * X + lax.rem(x + X - dx, X)

    def span(which, k, count=1):
        return pl.ds(pl.multiple_of(which * n + k * rows_here, align), count * rows_here)

    def remote(src, dst, send, recv, where):
        return pltpu.make_async_remote_copy(
            src_ref=src, dst_ref=dst, send_sem=send, recv_sem=recv,
            device_id=where, device_id_type=MESH,
        )

    def here(part, sem):
        return remote(part, part, sem, sem, plane_id(0, 0, 1))

    pairs = [(k, min(2, chunks - k)) for k in range(0, chunks, 2)]

    group_sizes = (1, len(lay.near), len(lay.far))

    def kind(i):
        return 0 if i < 0 else 1 if i in lay.near else 2

    def plane_copy(i, k):
        part = units.at[span(slot, k)]
        return remote(part, part, ps, pr.at[k // 2], plane_id(*lay.offsets[i], 0))

    def relay_copy(i, k):
        df, dx = lay.offsets[i]
        src, step = ((0, dx), (df, 0)) if k % 2 == 0 else ((df, 0), (0, dx))
        part = units.at[span(source_chip(*src) * C + core, k)]
        return remote(part, part, ps, fr.at[k // 2], plane_id(*step, 0))

    def sibling_copy(i, k, count):
        src = chip if i < 0 else source_chip(*lay.offsets[i])
        part = units.at[span(src * C + core, k, count)]
        return remote(part, part, ps, sr.at[kind(i)], plane_id(0, 0, 1))

    def near_wait(g):
        part = units.at[pl.ds(0, len(lay.near) * pairs[g][1] * rows_here)]
        here(part, pr.at[g]).wait_recv()

    def far_wait(g):
        part = units.at[pl.ds(0, len(lay.far) * pairs[g][1] * rows_here)]
        here(part, fr.at[g]).wait_recv()

    def sibling_wait(which):
        count = group_sizes[which]
        here(units.at[pl.ds(0, count * n)], sr.at[which]).wait_recv()

    sends_up = z < last
    sends_down = z == last
    relays_down = (z > 0) & (z < last - 1)

    def source(w):
        return last if w == 0 else z - w

    def valid(w, z=z):
        if w == 0:
            return (z < last - 1) & lay.down
        found = (z >= w) & (z < last)
        return (found | (z == last)) if w == 1 else found

    def goes_on(w, z=z):
        return (z >= w) & (z < last - 1)

    def results_of(src):
        return [(src + w, w) for w in range(1, lay.slots) if src + w < S and valid(w, src + w)] + [
            (there, 0) for there in range(S - 2) if src == last
        ]

    def place_of(w):
        found = jnp.int32(0)
        for there in range(S):
            if valid(w, there):
                owner = last if w == 0 else there - w
                found = jnp.where(z == there, results_of(owner).index((there, w)), found)
        return found

    def lr_at(w, k):
        return lr.at[w * chunks + (k if w < 2 or w != last - 1 else 0)]

    def line_copy(src, k, dst_slot, there):
        return remote(
            src, line.at[dst_slot, pl.ds(k * rows_here, rows_here)],
            ls, lr_at(dst_slot, k), line_id(there),
        )

    def own_part(k):
        return units.at[span(slot, k)]

    def slot_part(w, k):
        return line.at[w, pl.ds(k * rows_here, rows_here)]

    def own_up(k):
        return line_copy(own_part(k), k, 1, z + 1)

    held_back = list(range(early, chunks))
    depth = units.shape[1]
    by = len(held_back)
    cut = depth // by if by and depth % (by * LANES) == 0 else 0

    def held_part(row, k):
        if cut:
            return pl.ds(row + half, n - half), pl.ds((k - early) * cut, cut)
        return pl.ds(row + k * rows_here, rows_here), slice(None)

    tail_lead = [(0, k) for k in held_back[1:2] if C > 1] + [(C - 1, k) for k in held_back]
    tail_rest = [(0, k) for k in held_back if k not in held_back[1:2]] if C > 1 else []

    def tail_up(which, k):
        row = pl.multiple_of((chip * C + which) * n, LANES)
        where = {"row": (z + 1) * F + f, "col": x * C + which}
        return remote(
            units.at[held_part(row, k)], line.at[(1, *held_part(0, k))], ls, lr_at(1, k), where
        )

    def own_down(k):
        return line_copy(own_part(k), k, 0, z - 2)

    def relay_up(w, k):
        return line_copy(slot_part(w, k), k, w + 1, z + 1)

    def relay_down(k):
        return line_copy(slot_part(0, k), k, 0, z - 1)

    def line_wait(w, k):
        here(slot_part(w, k), lr_at(w, k)).wait_recv()

    def line_order(src, dst_slot, there):
        return remote(src, line_orders.at[dst_slot], los, lor.at[dst_slot], line_id(there))

    def order_up():
        return line_order(orders.at[slot], 1, z + 1)

    def order_down():
        return line_order(orders.at[slot], 0, z - 2)

    def order_on_up(w):
        return line_order(line_orders.at[w], w + 1, z + 1)

    def order_on_down():
        return line_order(line_orders.at[0], 0, z - 1)

    def order_send(src, sem, where):
        return remote(orders.at[src], orders.at[src], os_, sem, where)

    def order_copy(i):
        return order_send(slot, or_.at[0], plane_id(*lay.offsets[i], 0))

    def order_relay(i):
        df, dx = lay.offsets[i]
        return order_send(source_chip(0, dx) * C + core, or_.at[1], plane_id(df, 0, 0))

    def order_wait(which):
        here(orders.at[pl.ds(0, group_sizes[which])], or_.at[which - 1]).wait_recv()

    def order_across(i):
        src = chip if i < 0 else source_chip(*lay.offsets[i])
        return order_send(src * C + core, osr.at[kind(i)], plane_id(0, 0, 1))

    def order_across_wait(which):
        here(orders.at[pl.ds(0, group_sizes[which])], osr.at[which]).wait_recv()

    barrier = pltpu.get_barrier_semaphore()
    steps = [(*lay.offsets[i], 0) for i in lay.near] + ([(0, 0, 1)] if C > 1 else [])
    sides = ((z > 0, z - 1), (z < last, z + 1), (z == last - 2, z + 2))
    for step in steps:
        pl.semaphore_signal(barrier, inc=1, device_id=plane_id(*step), device_id_type=MESH)
    for there, which in sides:
        pl.when(there)(
            lambda which=which: pl.semaphore_signal(
                barrier, inc=1, device_id=line_id(which), device_id_type=MESH
            )
        )
    loads = [pltpu.make_async_copy(order, own_order, load.at[0])]
    for at, count in ((0, half), (half, n - half)):
        if count:
            rows = pl.ds(at, count)
            loads.append(pltpu.make_async_copy(emb.at[rows], raw.at[rows], load.at[len(loads)]))
    for one in loads:
        one.start()
    row_best[...] = jnp.full(row_best.shape, -1.0, jnp.float32)
    col_best[...] = jnp.full(col_best.shape, -1.0, jnp.float32)
    loads[0].wait()
    orders[pl.ds(slot, 1)] = own_order[...].reshape(1, 1, n)
    loads[1].wait()

    def normalize(k):
        floats = raw[pl.ds(k * rows_here, rows_here), :].astype(jnp.float32)
        scale = lax.rsqrt(jnp.sum(floats * floats, axis=1, keepdims=True) + 1e-06)
        units[span(slot, k), :] = (floats * scale).astype(jnp.bfloat16)

    for k in range(early):
        normalize(k)
    lines = jnp.minimum(z, 1) + jnp.minimum(last - z, 1)
    if lay.down:
        lines = lines + z // last
    pl.semaphore_wait(barrier, len(steps) + lines)

    def start(cond, *copies):
        @pl.when(cond)
        def run():
            for one in copies:
                one().start()

    holds = z == 1 if lay.hold else z < 0
    lead = core == C - 1
    if S > 1:
        start(sends_up, order_up, *[functools.partial(own_up, k) for k in range(early)])
    if half < n:
        loads[2].wait()
        for k in range(early, chunks):
            normalize(k)
    if half < n and S > 1:
        start(sends_up & jnp.logical_not(holds),
              *[functools.partial(own_up, k) for k in range(early, chunks)])
    if lay.down:
        start(sends_down, order_down, *[functools.partial(own_down, k) for k in range(chunks)])
    for i in lay.near:
        order_copy(i).start()
    if C > 1:
        order_across(-1).start()
    for k in range(chunks):
        for i in lay.near:
            plane_copy(i, k).start()
        if C > 1 and k == 0:
            sibling_copy(-1, 0, chunks).start()

    def spread(which, row):
        wide = jnp.broadcast_to(row.reshape(1, n), (LANES, n))
        col_orders[which] = wide.T

    spread(own, orders[slot])

    width = C * n

    def scores(lhs, first_chip, wide=1, depths=slice(None)):
        at = pl.multiple_of(first_chip * width, LANES)
        rhs = units[pl.ds(at, wide * width), depths]
        return lax.dot_general(
            lhs, rhs, (((1,), (1,)), ((), ())), preferred_element_type=jnp.float32
        )

    def fold(s, w, first_chip, both, first=0, count=n):
        mine = col_orders[w, first:first + count, :]
        rows_max = None
        for j in range(s.shape[1] // LANES):
            part = s[:, j * LANES:(j + 1) * LANES]
            which_chip, at = first_chip + j * LANES // width, j * LANES % width
            core_at, lane_at = at // n, at % n
            theirs = orders[which_chip * C + core_at, :, lane_at:lane_at + LANES]
            earlier = theirs < mine
            if both:
                cand = jnp.where(earlier, part, jnp.float32(-1.0))
                rows_max = cand if rows_max is None else jnp.maximum(rows_max, cand)
                later = jnp.where(earlier, jnp.float32(-1.0), part)
            else:
                later = jnp.where(mine < theirs, part, jnp.float32(-1.0))
            down = jnp.max(later.reshape(count // 8, 8, LANES), axis=0)
            col_best[which_chip, :, at:at + LANES] = jnp.maximum(
                col_best[which_chip, :, at:at + LANES], down
            )
        if both:
            row_best[w, first:first + count, :] = jnp.maximum(
                row_best[w, first:first + count, :], rows_max
            )

    def own_rows():
        return units[pl.ds(pl.multiple_of(slot * n, LANES), n), :]

    def own_item(which_chip):
        fold(scores(own_rows(), which_chip), own, which_chip, False)

    def run_all(jobs):
        ready = None
        for w, first, count, one in jobs:
            lhs = own_rows() if w == own else line[w, first:first + count, :]
            s = scores(lhs, one)
            if ready is not None:
                fold(*ready)
            ready = (s, w, one, w != own, first, count)
        if ready is not None:
            fold(*ready)

    def chips_of(places):
        def at(j):
            if places == "near":
                by_x = j < X - 1
                df = jnp.where(by_x, 0, j - (X - 2))
                dx = jnp.where(by_x, j + 1, 0)
            elif places == "far":
                df, dx = 1 + j // max(X - 1, 1), 1 + lax.rem(j, max(X - 1, 1))
            else:
                df, dx = 0, 0
            return source_chip(df, dx)

        return {"near": F + X - 2, "far": (F - 1) * (X - 1), "self": 1}[places], at

    def sweep(places, rows):
        count, at = chips_of(places)

        def step(j, carry):
            run_all([(*one, at(j)) for one in rows])
            return carry

        if count <= 2:
            run_all([(*one, at(j)) for j in range(count) for one in rows])
        else:
            lax.fori_loop(0, count, step, 0)

    def line_sweep(w, places, first, count, cond):
        pl.when(valid(w) & cond)(lambda: sweep(places, [(w, first, count)]))

    def sweep_own(places):
        sweep(places, [(own, 0, n)])

    wide = next(m for m in (4, 3, 2, 1) if lay.chips % m == 0)

    def wide_sweep(w, first, count, cond):
        def body(j, carry):
            s = scores(line[w, first:first + count, :], j * wide, wide)
            fold(s, w, j * wide, True, first, count)
            return carry

        @pl.when(valid(w) & cond)
        def run():
            lax.fori_loop(0, lay.chips // wide, body, 0)

    if lay.near:
        order_wait(1)
    if C > 1:
        for i in lay.near:
            order_across(i).start()
    for i in lay.far:
        order_relay(i).start()

    def take_order(w, cond):
        @pl.when(cond)
        def run():
            here(line_orders.at[w], lor.at[w]).wait_recv()
            if w == 0:
                pl.when(relays_down)(lambda: order_on_down().start())
            elif w < last - 1:
                pl.when(goes_on(w))(lambda: order_on_up(w).start())
            spread(w, line_orders[w])

    if S > 1:
        take_order(1, valid(1))
    if C > 1:
        order_across_wait(0)
        sibling_wait(0)
    own_item(chip)
    held = z == 2 if lay.hold else z < 0
    straight = jnp.logical_not(held)

    def take(w, k, cond):
        @pl.when(cond)
        def run():
            line_wait(w, k)
            if w < last - 1:
                pl.when(goes_on(w))(lambda: relay_up(w, k).start())

    def take_down(p):
        for there in range(S - 3, 0, -1):
            k = p - 1 - 2 * (S - 3 - there)
            if k == 0:
                take_order(0, z == there)
            if 0 <= k < chunks:
                @pl.when(z == there)
                def run(k=k):
                    line_wait(0, k)
                    relay_down(k).start()

    def far_group(g):
        if lay.far:
            far_wait(g)
        if C > 1:
            for i in lay.far:
                sibling_copy(i, *pairs[g]).start()

    def near_group(g):
        if lay.near:
            near_wait(g)
        for k in range(pairs[g][0], sum(pairs[g])):
            for i in lay.far:
                relay_copy(i, k).start()
        if C > 1:
            for i in lay.near:
                sibling_copy(i, *pairs[g]).start()

    for p in range(chunks + 2 * max(S - 4, 0) + 1):
        if p < chunks and S > 1:
            take(1, p, valid(1) if p < early else valid(1) & straight)
        for w in range(2, last - 1):
            k = p - 2 * (w - 1)
            if k == 0:
                take_order(w, goes_on(w))
            if 0 <= k < chunks:
                take(w, k, goes_on(w))
        if lay.hold and p == chunks - 1:
            if tail_rest:
                start(holds & (core == 0), *[functools.partial(tail_up, *one) for one in tail_rest])
        take_down(p)
        if p < chunks and (p % 2 or p == chunks - 1):
            near_group(p // 2)
        if lay.hold and p == early + 1:
            line_sweep(1, "self", 0, half, held)
    if C > 1:
        if lay.near:
            order_across_wait(1)
            sibling_wait(1)
    sweep_own("near")
    if lay.far:
        order_wait(2)
    if C > 1:
        for i in lay.far:
            order_across(i).start()
    far_group(0)
    ends = z == last - 1
    bottom = z == 0

    def line_result(w):
        return remote(line_res.at[w], line_in.at[place_of(w)], lrs, lrr, line_id(source(w)))

    def give_back(w, cond):
        @pl.when(valid(w) & cond)
        def run():
            line_res[w] = jnp.max(row_best[w].T, axis=0, keepdims=True)
            line_result(w).start()

    def take_rows(w, cond):
        @pl.when(valid(w) & cond)
        def run():
            if w > 1 and w == last - 1:
                here(line.at[w], lr_at(w, 0)).wait_recv()
            else:
                for k in range(chunks):
                    line_wait(w, k)
        take_order(w, valid(w) & cond)

    if lay.hold:
        start(holds & lead, *[functools.partial(tail_up, *one) for one in tail_lead])
    if S > 1:
        line_sweep(1, "self", 0, n, straight)
        if lay.hold:
            line_sweep(1, "near", 0, half, held)
    if lay.down:
        line_sweep(0, "self", 0, n, relays_down)
    for g in range(1, len(pairs) - 1):
        far_group(g)
    if lay.down:
        take_rows(0, bottom)
        line_sweep(0, "self", 0, n, bottom)
    for g in range(max(len(pairs) - 1, 1), len(pairs)):
        far_group(g)
    for w in range(2, last):
        take_rows(w, ends)
        line_sweep(w, "self", 0, n, z < last if not lay.hold else lead)
    if S > 1:
        line_sweep(1, "near", 0, n, straight)
    for w in range(2, last):
        line_sweep(w, "near", 0, n, z < last if not lay.hold else lead)
    if lay.down:
        line_sweep(0, "near", 0, n, valid(0))
    if C > 1:
        if lay.far:
            order_across_wait(2)
            sibling_wait(2)
    if lay.hold:
        line_sweep(2, "far", 0, n, lead)
        if C > 1:
            wide_sweep(2, 0, n, core == 0)
        give_back(2, z < last)
        pl.when(held)(lambda: sweep("far", [(own, 0, n), (1, 0, half)]))
        pl.when(z == 1)(lambda: sweep("far", [(own, 0, n), (0, 0, n), (1, 0, n)]))
        pl.when(z == last)(lambda: sweep("far", [(own, 0, n), (1, 0, n)]))
        pl.when(bottom)(lambda: sweep("far", [(own, 0, n), (0, 0, n)]))
    else:
        sweep_own("far")
        for w in range(2, last):
            line_sweep(w, "far", 0, n, z < last)
        if lay.down:
            line_sweep(0, "far", 0, n, valid(0))
        if S > 1:
            line_sweep(1, "far", 0, n, straight)
    for w in range(2, 2 if lay.hold else last):
        give_back(w, z < last)
    if S > 1:
        give_back(1, straight)
    if lay.down:
        give_back(0, valid(0))
    tail = half // LANES * LANES
    rest = slice((by - 1) * cut, None) if cut else slice(None)

    def take_held(k):
        @pl.when(held)
        def run():
            here(line.at[(1, *held_part(0, k))], lr_at(1, k)).wait_recv()

    def places():
        return [(j // X, j % X) for j in range(lay.chips - 1, -1, -1)]

    def chip_at(df, dx):
        return lax.rem(f + df, F) * X + lax.rem(x + dx, X)

    def begin_late(first, stop):
        depths = slice(first * cut, stop * cut)
        for j, place in enumerate(places()):
            s = scores(line[1, half:, depths], chip_at(*place), 1, depths)
            sums[j] = s + sums[j] if first else s

    if lay.hold:
        if tail:
            @pl.when(held)
            def run():
                line_res[1, :, :tail] = jnp.max(row_best[1, :tail, :].T, axis=0, keepdims=True)
        ahead = cut and lay.chips <= 4
        for k in held_back[:-1]:
            take_held(k)
            if ahead:
                pl.when(held & lead)(lambda k=k: begin_late(k - early, k - early + 1))
        if ahead and C > 1 and by > 1:
            pl.when(held & (core == 0))(lambda: begin_late(0, by - 1))
        take_held(held_back[-1])

    def result_copy(df, dx, dc):
        there = (lax.rem(f + df, F) * X + lax.rem(x + dx, X)) * C + lax.rem(core + dc, C)
        o = (df * X + dx) * C + dc
        return remote(plane_res.at[there], plane_in.at[o], rs, rr, plane_id(df, dx, dc))

    def flush(df, dx):
        one = lax.rem(f + df, F) * X + lax.rem(x + dx, X)
        flat = jnp.max(col_best[one], axis=0, keepdims=True)
        for core_at in range(C):
            plane_res[one * C + core_at] = flat[:, core_at * n:(core_at + 1) * n]

    def flush_out(df, dx, first=0):
        flush(df, dx)
        for dc in range(first, C):
            result_copy(df, dx, dc).start()

    def finish():
        def step(j, carry):
            flush_out((lay.chips - 1 - j) // X, lax.rem(lay.chips - 1 - j, X))
            return carry

        if lay.chips > 4:
            lax.fori_loop(0, lay.chips - 1, step, 0)
        else:
            for j in range(lay.chips - 1, 0, -1):
                flush_out(j // X, j % X)
        flush_out(0, 0, 1)

    def finish_late():
        ready = None

        def settle():
            s, at, place = ready
            fold(s, 1, at, True, half, n - half)
            if place != (0, 0):
                flush_out(*place)

        for j, place in enumerate(places()):
            s = scores(line[1, half:, rest], chip_at(*place), 1, rest)
            if cut:
                s = s + sums[j]
            if ready is not None:
                settle()
            ready = s, chip_at(*place), place
        settle()
        line_res[1, :, tail:] = jnp.max(row_best[1, tail:, :].T, axis=0, keepdims=True)
        line_result(1).start()
        flush_out(0, 0, 1)

    if lay.hold and lay.chips <= 4:
        pl.when(held)(finish_late)
        pl.when(straight)(finish)
    elif lay.hold:
        wide_sweep(1, half, n - half, held)
        give_back(1, held)
        finish()
    else:
        finish()

    def sent(part, sem):
        here(part, sem).wait_send()

    if lay.plane > 1:
        sent(units.at[pl.ds(0, (lay.plane - 1) * n)], ps)
        sent(orders.at[pl.ds(0, lay.plane - 1)], os_)

    def line_sent(cond, pieces, copies, results):
        @pl.when(cond)
        def run():
            if pieces:
                sent(units.at[pl.ds(0, pieces * rows_here)], ls)
            if copies:
                sent(orders.at[pl.ds(0, copies)], los)
            if results:
                sent(plane_in.at[pl.ds(0, results)], lrs)

    for there in range(S):
        moved = sum(bool(goes_on(w, there)) for w in range(1, last - 1))
        moved += bool(lay.down and 0 < there < last - 1)
        owns = there < last or lay.down
        results = sum(bool(valid(w, there)) for w in range(lay.slots))
        if S == 1:
            continue
        if lay.hold and there == 1:
            for cond, held_pieces in ((lead, tail_lead), (jnp.logical_not(lead), tail_rest)):
                pieces = early + moved * chunks + len(held_pieces)
                line_sent((z == there) & cond, pieces, moved + owns, results)
        else:
            line_sent(z == there, (moved + owns) * chunks, moved + owns, results)

    best = jnp.maximum(plane_res[slot], jnp.float32(-1.0))
    if lay.plane > 1:
        here(plane_in.at[pl.ds(1, lay.plane - 1)], rr).wait_recv()
        best = jnp.maximum(best, jnp.max(plane_in[1:], axis=0))
    plane_res[slot] = best
    for there in range(S):
        count = len(results_of(there))
        if count:
            @pl.when(z == there)
            def run(count=count):
                part = line_in.at[pl.ds(0, count)]
                here(part, lrr).wait_recv()
                plane_res[slot] = jnp.maximum(plane_res[slot], jnp.max(part[...], axis=0))
    out[...] = plane_res[slot].reshape(n)
    if lay.plane > 1:
        sent(plane_in.at[pl.ds(1, lay.plane - 1)], rs)


def shards(lay, embeddings, doc_order):
    n, depth = embeddings.shape
    chunks = n // PIECE if n % PIECE == 0 else 1
    dma = pltpu.SemaphoreType.DMA
    S = lay.slow
    pieces = chunks * (lay.slots - lay.hold) + lay.hold
    vmem = pltpu.VMEM
    return pl.pallas_call(
        functools.partial(kernel, lay, n, chunks),
        out_shape=vmem((n,), jnp.float32),
        in_specs=[pl.BlockSpec(memory_space=pl.ANY)] * 2,
        out_specs=pl.BlockSpec(memory_space=vmem),
        scratch_shapes=[
            vmem((n, depth), jnp.bfloat16),
            vmem((n,), jnp.int32),
            vmem((lay.plane * n, depth), jnp.bfloat16),
            vmem((lay.slots, n, depth), jnp.bfloat16),
            vmem((lay.plane, 1, n), jnp.int32),
            vmem((lay.slots, 1, n), jnp.int32),
            vmem((lay.slots + 1, n, LANES), jnp.int32),
            vmem((min(lay.chips, 4), n // 2, lay.cores * n), jnp.float32),
            vmem((lay.slots, n, LANES), jnp.float32),
            vmem((lay.chips, 8, lay.cores * n), jnp.float32),
            vmem((lay.plane, 1, n), jnp.float32),
            vmem((lay.slots, 1, n), jnp.float32),
            vmem((lay.plane, 1, n), jnp.float32),
            vmem((S, 1, n), jnp.float32),
            dma((3,)),
            dma(()), dma(((chunks + 1) // 2,)), dma(((chunks + 1) // 2,)), dma((3,)),
            dma(()), dma((pieces,)),
            dma(()), dma((2,)), dma((3,)),
            dma(()), dma((lay.slots,)),
            dma(()), dma(()),
            dma(()), dma(()),
        ],
        compiler_params=pltpu.CompilerParams(
            collective_id=0, has_side_effects=True, vmem_limit_bytes=60 * 1024 * 1024
        ),
    )(embeddings, doc_order)


def solution(mesh):
    lay = Layout(mesh.shape["row"], mesh.shape["col"])
    return jax.shard_map(
        functools.partial(shards, lay),
        mesh=mesh,
        in_specs=(P(("row", "col"), None), P(("row", "col"))),
        out_specs=P(("row", "col")),
        check_vma=False,
    )
```
